32 devices in a mesh: replica: 4 (over x, core), shard: 8 (over z, y).
Axes of the slice: x: 2, y: 2, z: 4, core: 2. Of those that a mesh axis runs over, the one named last changes fastest.
Arguments:
- block_input: bfloat16 [8192, 2048], P(('replica', 'shard')), may hold values from -6 to 6
- segment_ids: int32 [32, 256], P(('replica', 'shard')), may hold values from 0 to 3, never falling along the last dimension, each value on 1 to 128 neighbouring positions
- attn_gain: bfloat16 [2048], P('shard'), may hold values from 0.5 to 1.5
- mlp_gain: bfloat16 [2048], P('shard'), may hold values from 0.5 to 1.5
- w_query: bfloat16 [2048, 2048], P('shard'), may hold values from -0.125 to 0.125
- w_key: bfloat16 [2048, 2048], P('shard'), may hold values from -0.125 to 0.125
- w_value: bfloat16 [2048, 2048], P('shard'), may hold values from -0.125 to 0.125
- w_out: bfloat16 [2048, 2048], P('shard'), may hold values from -0.5 to 0.5
- w_gate: bfloat16 [2048, 8192], P('shard'), may hold values from -0.125 to 0.125
- w_up: bfloat16 [2048, 8192], P('shard'), may hold values from -0.125 to 0.125
- w_down: bfloat16 [8192, 2048], P('shard'), may hold values from -0.0625 to 0.0625
- out_grad: bfloat16 [8192, 2048], P(('replica', 'shard')), may hold values from -6 to 6
Outputs:
- block_output: bfloat16 [8192, 2048], P(('replica', 'shard'))
- input_grad: float32 [8192, 2048], P(('replica', 'shard'))
- grad_query: float32 [2048, 2048], P('shard')
- grad_key: float32 [2048, 2048], P('shard')
- grad_value: float32 [2048, 2048], P('shard')
- grad_out: float32 [2048, 2048], P('shard')
- grad_gate: float32 [2048, 8192], P('shard')
- grad_up: float32 [2048, 8192], P('shard')
- grad_down: float32 [8192, 2048], P('shard')
- grad_attn_gain: float32 [2048], P('shard')
- grad_mlp_gain: float32 [2048], P('shard')
The draws below stay inside these ranges and needn't reach their ends.
Inputs may be any that keep to these rules, and one draw needn't show every extreme that they name: `segment_ids`: along each packed row the ids never fall; every document holds 1 to 128 tokens and one holds exactly 128.
All inputs are finite; a program needn't handle non-finite values.
Results may differ from the reference program's by a relative error of at most 0.02.
Values may be sent and summed in bfloat16 or wider, within the bound.
A program may use at most 640 MiB of HBM per device.

```python
import math
import jax
import jax.numpy as jnp
import numpy as np
from jax import lax

D = 2048
FF = 8192
HEAD_DIM = 64
TOK_DEV = 256
PACKS = 32
TOKENS = 8192
SEGMENTS = 4
MOST = 128


def block_scale(key, shape, split, least, high):
    factor_of, own = 1.0, jax.random.fold_in(key, 6)
    for dim, parts in split:
        steps = jnp.exp(jax.random.uniform(jax.random.fold_in(own, dim), (parts,), jnp.float32, least / len(split), high / len(split)))
        factor_of = factor_of * jnp.repeat(steps, shape[dim] // parts).reshape([-1 if axis == dim else 1 for axis in range(len(shape))])
    return factor_of


def split_up(amount, total, bound, lean):
    loads = [(1 << 20) // math.isqrt(standing ** lean) + 1 for standing in range(2, amount + 1)]
    rest, counts = total - bound - (amount - 1), [1] * (amount - 1)
    while rest > 0:
        movable = [i for i in range(amount - 1) if counts[i] < bound]
        whole, remaining = sum([loads[i] for i in movable]), rest
        for i in movable:
            more = min(bound - counts[i], max(1, remaining * loads[i] // whole), rest)
            counts[i] = counts[i] + more
            rest = rest - more
    return np.array([bound] + counts)


def uneven(own_key, amount, total, most, skew):
    if amount == 2:
        one = jax.random.randint(own_key, (), max(1, total - most), min(most, total - 1) + 1)
        return jnp.stack([one, total - one])
    lengths = jnp.asarray(split_up(amount, total, most, skew), jnp.int32)
    twos = (amount - 1) // 2
    source_of, taker = lengths[1:1 + 2 * twos:2], lengths[2:2 + 2 * twos:2]
    margin = jnp.minimum(source_of - 1, most - taker)
    moved = jax.random.randint(jax.random.fold_in(own_key, 1), (twos,), 0, 1 << 20) % (margin + 1)
    lengths = lengths.at[1:1 + 2 * twos:2].set(source_of - moved).at[2:2 + 2 * twos:2].set(taker + moved)
    return lengths[jax.random.permutation(jax.random.fold_in(own_key, 2), amount)]


def normal_values(own_key, dims, width, most, split=(), kind=jnp.bfloat16):
    drawn = jax.random.normal(own_key, dims, jnp.float32) * width
    if len(split) > 0:
        drawn = block_scale(own_key, dims, split, -0.22, 0.18) * drawn
    return jnp.clip(drawn, min=-most, max=most).astype(kind)


def setup_inputs(seed: int = 0) -> dict:
    arg_keys = jax.random.split(jax.random.key(seed), 13)
    return {
        "block_input": normal_values(arg_keys[0], (TOKENS, D), 1.0, 6.0, ((0, 32),)),
        "segment_ids": jax.vmap(lambda own: jnp.searchsorted(jnp.cumsum(uneven(own, SEGMENTS, TOK_DEV, MOST, 1)), jnp.arange(TOK_DEV), side="right"))(jax.random.split(arg_keys[1], PACKS)).reshape((PACKS, TOK_DEV)).astype(jnp.int32),
        "attn_gain": jnp.clip(1.0 + 0.1 * jax.random.normal(arg_keys[2], (D,), jnp.float32), 0.5, 1.5).astype(jnp.bfloat16),
        "mlp_gain": jnp.clip(1.0 + 0.1 * jax.random.normal(arg_keys[3], (D,), jnp.float32), 0.5, 1.5).astype(jnp.bfloat16),
        "w_query": normal_values(arg_keys[4], (D, D), D ** -0.5, 0.125, ((0, 8),)),
        "w_key": normal_values(arg_keys[5], (D, D), D ** -0.5, 0.125, ((0, 8),)),
        "w_value": normal_values(arg_keys[6], (D, D), D ** -0.5, 0.125, ((0, 8),)),
        "w_out": normal_values(arg_keys[7], (D, D), (D // 16) ** -0.5, 0.5, ((0, 8),)),
        "w_gate": normal_values(arg_keys[8], (D, FF), D ** -0.5, 0.125, ((0, 8),)),
        "w_up": normal_values(arg_keys[9], (D, FF), D ** -0.5, 0.125, ((0, 8),)),
        "w_down": normal_values(arg_keys[10], (FF, D), FF ** -0.5, 0.0625, ((0, 8),)),
        "out_grad": normal_values(arg_keys[11], (TOKENS, D), 1.0, 6.0, ((0, 32),)),
    }


EPS = 1e-05
THETA = 130000.0
SCALE = 0.125

def round_trip(values):
    return lax.optimization_barrier(values.astype(jnp.bfloat16)).astype(jnp.float32)

def positions_tables(segment_row, head_dim):
    length_all = segment_row.shape[0]
    counter = jnp.arange(length_all, dtype=jnp.int32)
    is_first = jnp.concatenate([jnp.ones((1,), jnp.bool_), segment_row[1:] != segment_row[:-1]])
    first_at = lax.cummax(jnp.where(is_first, counter, jnp.zeros_like(counter)), axis=0)
    position = (counter - first_at).astype(jnp.float32)
    half_dim = head_dim // 2
    inverse = jnp.exp(-(jnp.arange(half_dim, dtype=jnp.float32) * (2.0 / head_dim)) * math.log(THETA))
    angles = position[:, None] * inverse[None, :]
    return (jnp.cos(angles), jnp.sin(angles))

def rotate(values, cosine, sine_tab, direction, head_dim):
    row_count, total_width = values.shape
    half_dim = head_dim // 2
    halves = values.reshape(row_count, total_width // head_dim, 2, half_dim)
    first_half = halves[:, :, 0]
    second_half = halves[:, :, 1]
    cos_wide = cosine[:, None, :]
    sin_wide = direction * sine_tab[:, None, :]
    turned = jnp.stack([first_half * cos_wide - second_half * sin_wide, second_half * cos_wide + first_half * sin_wide], axis=2)
    return turned.reshape(row_count, total_width)

def allowed(segment_row, row_start, span_rows):
    length_all = segment_row.shape[0]
    row_ids = row_start + jnp.arange(span_rows, dtype=jnp.int32)
    col_ids = jnp.arange(length_all, dtype=jnp.int32)
    seg_rows = lax.dynamic_slice_in_dim(segment_row, row_start, span_rows)
    return (seg_rows[:, None] == segment_row[None, :]) & (col_ids[None, :] <= row_ids[:, None])

def attention_forward(q_rot, k_rot, v_vals, segment_row, head_dim):
    row_count, total_width = q_rot.shape
    n_heads = total_width // head_dim
    span_rows = min(512, row_count)
    q_heads = q_rot.astype(jnp.float32).reshape(row_count, n_heads, head_dim)
    k_heads = k_rot.astype(jnp.float32).reshape(row_count, n_heads, head_dim)
    v_heads = v_vals.astype(jnp.float32).reshape(row_count, n_heads, head_dim)

    def one_block(block_id):
        row_start = block_id * span_rows
        q_block = lax.dynamic_slice_in_dim(q_heads, row_start, span_rows, 0)
        scores = jnp.einsum('qhd,khd->hqk', q_block, k_heads) * SCALE
        scores = jnp.where(allowed(segment_row, row_start, span_rows)[None], scores, -1e+30)
        log_total = jnp.log(lax.optimization_barrier(jnp.sum(jnp.exp(scores), axis=-1)))
        rounded_probs = round_trip(jnp.exp(scores - log_total[..., None]))
        mixed_out = jnp.einsum('hqk,khd->qhd', rounded_probs, v_heads)
        return (mixed_out.astype(jnp.bfloat16).reshape(span_rows, total_width), log_total)
    outputs, log_totals = lax.map(one_block, jnp.arange(row_count // span_rows, dtype=jnp.int32))
    return (outputs.reshape(row_count, total_width), log_totals.transpose(1, 0, 2).reshape(n_heads, row_count))

def attention_backward(q_rot, k_rot, v_vals, log_totals, grad_att, segment_row, head_dim):
    row_count, total_width = q_rot.shape
    n_heads = total_width // head_dim
    span_rows = min(512, row_count)
    q_heads = q_rot.astype(jnp.float32).reshape(row_count, n_heads, head_dim)
    k_heads = k_rot.astype(jnp.float32).reshape(row_count, n_heads, head_dim)
    v_heads = v_vals.astype(jnp.float32).reshape(row_count, n_heads, head_dim)
    g_heads = grad_att.astype(jnp.float32).reshape(row_count, n_heads, head_dim)

    def one_block(carried, block_id):
        key_acc, value_acc = carried
        row_start = block_id * span_rows
        q_block = lax.dynamic_slice_in_dim(q_heads, row_start, span_rows, 0)
        g_block = lax.dynamic_slice_in_dim(g_heads, row_start, span_rows, 0)
        lse_block = lax.dynamic_slice_in_dim(log_totals, row_start, span_rows, 1)
        scores = jnp.einsum('qhd,khd->hqk', q_block, k_heads) * SCALE
        scores = jnp.where(allowed(segment_row, row_start, span_rows)[None], scores, -1e+30)
        attn_probs = jnp.exp(scores - lse_block[..., None])
        grad_probs = jnp.einsum('qhd,khd->hqk', g_block, v_heads)
        inner_sum = lax.optimization_barrier(jnp.sum(attn_probs * grad_probs, axis=-1, keepdims=True))
        grad_scores = round_trip(attn_probs * (grad_probs - inner_sum) * SCALE)
        rounded_probs = round_trip(attn_probs)
        grad_query = jnp.einsum('hqk,khd->qhd', grad_scores, k_heads)
        key_acc = key_acc + jnp.einsum('hqk,qhd->khd', grad_scores, q_block)
        value_acc = value_acc + jnp.einsum('hqk,qhd->khd', rounded_probs, g_block)
        return ((key_acc, value_acc), grad_query.reshape(span_rows, total_width))
    zeros_heads = jnp.zeros((row_count, n_heads, head_dim), jnp.float32)
    (key_acc, value_acc), grad_blocks = lax.scan(one_block, (zeros_heads, zeros_heads), jnp.arange(row_count // span_rows, dtype=jnp.int32))
    return (grad_blocks.reshape(row_count, total_width), key_acc.reshape(row_count, total_width), value_acc.reshape(row_count, total_width))

def matmul(left_op, right_op):
    return jnp.dot(left_op, right_op, preferred_element_type=jnp.float32)

def one_pack(block_input, segment_row, out_grad, attn_gain, mlp_gain, w_query, w_key, w_value, w_out, w_gate, w_up, w_down):
    cosine, sine_tab = positions_tables(segment_row, HEAD_DIM)
    input_f = block_input.astype(jnp.float32)
    scale_one = lax.rsqrt(lax.optimization_barrier(jnp.mean(input_f * input_f, axis=-1, keepdims=True)) + EPS)
    gain_one = attn_gain.astype(jnp.float32)
    normed_one = (input_f * scale_one * gain_one).astype(jnp.bfloat16)
    query_proj = matmul(normed_one, w_query)
    key_proj = matmul(normed_one, w_key)
    value_proj = matmul(normed_one, w_value)
    q_rot = rotate(query_proj, cosine, sine_tab, 1.0, HEAD_DIM).astype(jnp.bfloat16)
    k_rot = rotate(key_proj, cosine, sine_tab, 1.0, HEAD_DIM).astype(jnp.bfloat16)
    v_vals = value_proj.astype(jnp.bfloat16)
    attended, log_totals = attention_forward(q_rot, k_rot, v_vals, segment_row, HEAD_DIM)
    residual = input_f + matmul(attended, w_out)
    scale_two = lax.rsqrt(lax.optimization_barrier(jnp.mean(residual * residual, axis=-1, keepdims=True)) + EPS)
    gain_two = mlp_gain.astype(jnp.float32)
    normed_two = (residual * scale_two * gain_two).astype(jnp.bfloat16)
    gate_pre = matmul(normed_two, w_gate)
    up_pre = matmul(normed_two, w_up)
    gate_sig = jax.nn.sigmoid(gate_pre)
    silu_val = gate_pre * gate_sig
    hidden_b = (silu_val * up_pre).astype(jnp.bfloat16)
    block_output = (residual + matmul(hidden_b, w_down)).astype(jnp.bfloat16)
    grad_out_f = out_grad.astype(jnp.float32)
    grad_hidden = matmul(out_grad, w_down.T)
    down_term = matmul(hidden_b.T, out_grad)
    gate_b = (grad_hidden * up_pre * gate_sig * (1.0 + gate_pre * (1.0 - gate_sig))).astype(jnp.bfloat16)
    up_b = (grad_hidden * silu_val).astype(jnp.bfloat16)
    gate_term = matmul(normed_two.T, gate_b)
    up_term = matmul(normed_two.T, up_b)
    grad_normed_two = matmul(gate_b, w_gate.T) + matmul(up_b, w_up.T)
    gain_two_term = lax.optimization_barrier(jnp.sum(grad_normed_two * residual * scale_two, axis=0))
    weighted_two = gain_two * grad_normed_two
    grad_residual = grad_out_f + scale_two * weighted_two - residual * (scale_two * scale_two * scale_two) * lax.optimization_barrier(jnp.mean(weighted_two * residual, axis=-1, keepdims=True))
    residual_b = grad_residual.astype(jnp.bfloat16)
    out_term = matmul(attended.T, residual_b)
    grad_att = matmul(residual_b, w_out.T).astype(jnp.bfloat16)
    grad_q, grad_k, grad_v = attention_backward(q_rot, k_rot, v_vals, log_totals, grad_att, segment_row, HEAD_DIM)
    q_back = rotate(grad_q, cosine, sine_tab, -1.0, HEAD_DIM).astype(jnp.bfloat16)
    k_back = rotate(grad_k, cosine, sine_tab, -1.0, HEAD_DIM).astype(jnp.bfloat16)
    v_back = grad_v.astype(jnp.bfloat16)
    query_term = matmul(normed_one.T, q_back)
    key_term = matmul(normed_one.T, k_back)
    value_term = matmul(normed_one.T, v_back)
    grad_normed_one = matmul(q_back, w_query.T) + matmul(k_back, w_key.T) + matmul(v_back, w_value.T)
    gain_one_term = lax.optimization_barrier(jnp.sum(grad_normed_one * input_f * scale_one, axis=0))
    weighted_one = gain_one * grad_normed_one
    input_grad = grad_residual + scale_one * weighted_one - input_f * (scale_one * scale_one * scale_one) * lax.optimization_barrier(jnp.mean(weighted_one * input_f, axis=-1, keepdims=True))
    terms = (query_term, key_term, value_term, out_term, gate_term, up_term, down_term, gain_one_term, gain_two_term)
    return (block_output, input_grad, terms)

def reference(block_input, segment_ids, attn_gain, mlp_gain, w_query, w_key, w_value, w_out, w_gate, w_up, w_down, out_grad):
    pack_count, pack_rows = segment_ids.shape
    model_width = block_input.shape[1]
    inputs_packed = block_input.reshape(pack_count, pack_rows, model_width)
    cotan_packed = out_grad.reshape(pack_count, pack_rows, model_width)

    def pack_step(carried, packed):
        input_pack, segment_pack, cotan_pack = packed
        output_pack, input_grad_pack, terms = one_pack(input_pack, segment_pack, cotan_pack, attn_gain, mlp_gain, w_query, w_key, w_value, w_out, w_gate, w_up, w_down)
        return (tuple((running + term_now for running, term_now in zip(carried, terms))), (output_pack, input_grad_pack))
    initial = (jnp.zeros(w_query.shape, jnp.float32), jnp.zeros(w_key.shape, jnp.float32), jnp.zeros(w_value.shape, jnp.float32), jnp.zeros(w_out.shape, jnp.float32), jnp.zeros(w_gate.shape, jnp.float32), jnp.zeros(w_up.shape, jnp.float32), jnp.zeros(w_down.shape, jnp.float32), jnp.zeros((model_width,), jnp.float32), jnp.zeros((model_width,), jnp.float32))
    totals, (outputs, input_grads) = lax.scan(pack_step, initial, (inputs_packed, segment_ids, cotan_packed))
    return (outputs.reshape(pack_count * pack_rows, model_width), input_grads.reshape(pack_count * pack_rows, model_width), totals[0], totals[1], totals[2], totals[3], totals[4], totals[5], totals[6], totals[7], totals[8])
```

```python
import functools
import math

import jax
import jax.numpy as jnp
from jax import lax
from jax.experimental import pallas as pl
from jax.experimental.pallas import tpu as pltpu
from jax.sharding import PartitionSpec as P

MESH = pl.DeviceIdType.MESH

HEAD_DIM = 64


EPS = 1e-05
THETA = 130000.0
SCALE = 0.125


def times_plain(left_op, right_op):
    return jnp.dot(left_op, right_op, preferred_element_type=jnp.float32)


def times_transposed(left_op, right_op):
    return lax.dot_general(
        left_op, right_op, (((1,), (1,)), ((), ())), preferred_element_type=jnp.float32
    )


def token_contract(left_op, right_op):
    return lax.dot_general(
        left_op, right_op, (((0,), (0,)), ((), ())), preferred_element_type=jnp.float32
    )


def split_rows(rows):
    unit = 16
    across = (rows // unit) * 3 // 16 * unit
    rest = (rows - across) // unit
    count = min(4, rest)
    sizes = [(rest // count + (1 if i >= count - rest % count else 0)) * unit for i in range(count)]
    chunks, at = [], across
    for size in sizes:
        chunks.append((at, size))
        at += size
    return across, chunks


def use_kernels(n, rows):
    return n % 2 == 0 and 2 < n <= 8 and rows % 256 == 0


def wire_cost(size):
    return pl.CostEstimate(flops=0, bytes_accessed=30 * size, transcendentals=0)


class Copies:
    def __init__(self):
        self.started = []

    def start(self, cond, src, dst, send_sem, recv_sem, target, axis="shard"):
        copy = pltpu.make_async_remote_copy(
            src_ref=src,
            dst_ref=dst,
            send_sem=send_sem,
            recv_sem=recv_sem,
            device_id={axis: target},
            device_id_type=MESH,
        )
        if cond is None:
            copy.start()
        else:
            pl.when(cond)(copy.start)
        self.started.append((cond, copy))

    def finish(self):
        for cond, copy in self.started:
            if cond is None:
                copy.wait_send()
            else:
                pl.when(cond)(copy.wait_send)


def wait_arrival(dst, send_sem, recv_sem, source, axis="shard"):
    pltpu.make_async_remote_copy(
        src_ref=dst,
        dst_ref=dst,
        send_sem=send_sem,
        recv_sem=recv_sem,
        device_id={axis: source},
        device_id_type=MESH,
    ).wait_recv()


def greet(has_left, has_right, left, right, other):
    barrier = pltpu.get_barrier_semaphore()
    pl.semaphore_signal(barrier, inc=1, device_id={"shard": other}, device_id_type=MESH)

    @pl.when(has_left)
    def _():
        pl.semaphore_signal(barrier, inc=1, device_id={"shard": left}, device_id_type=MESH)

    @pl.when(has_right)
    def _():
        pl.semaphore_signal(barrier, inc=1, device_id={"shard": right}, device_id_type=MESH)

    pl.semaphore_wait(barrier, 1 + has_left.astype(jnp.int32) + has_right.astype(jnp.int32))


def gather_kernel(n, across, chunks, x_ref, o_ref, own_sem, z_send, z_recv, y_send, y_recv):
    length = n // 2
    count = len(chunks)
    me = lax.axis_index("shard")
    place, side = me // 2, me % 2
    other = me + 1 - 2 * side
    has_left, has_right = place > 0, place < length - 1
    nexts = ((has_right, me + 2), (has_left, me - 2))
    greet(has_left, has_right, me - 2, me + 2, other)
    copies = Copies()
    own = pltpu.make_async_copy(x_ref, o_ref.at[me], own_sem)
    own.start()
    first = pl.ds(0, across)
    y_first = (2 * length - 1) * count
    copies.start(
        None, x_ref.at[first], o_ref.at[me, first], y_send.at[y_first], y_recv.at[y_first], other
    )

    def z_hop(direction, hop, slot, src, dst):
        cond, target = nexts[direction]
        copies.start(
            cond,
            src,
            dst,
            z_send.at[direction, hop, slot],
            z_recv.at[direction, hop, slot],
            target,
        )

    def y_hop(origin, chunk, src, dst, cond, key):
        copies.start(cond, src, dst, y_send.at[key], y_recv.at[key], other)

    for c, (at, size) in enumerate(chunks):
        span = pl.ds(at, size)
        for direction in range(2):
            z_hop(direction, 0, c, x_ref.at[span], o_ref.at[me, span])
        y_hop(me, c, x_ref.at[span], o_ref.at[me, span], None, c)
    for hop in range(1, length):
        for c, (at, size) in enumerate(chunks):
            span = pl.ds(at, size)
            for direction in range(2):
                source = me - 2 * hop if direction == 0 else me + 2 * hop
                exists = source >= 0 if direction == 0 else source < n
                sender = me - 2 if direction == 0 else me + 2

                @pl.when(exists)
                def _():
                    wait_arrival(
                        o_ref.at[source, span],
                        z_send.at[direction, hop - 1, c],
                        z_recv.at[direction, hop - 1, c],
                        sender,
                    )

                here = o_ref.at[source, span]
                if hop < length - 1:
                    cond, target = nexts[direction]
                    copies.start(
                        jnp.logical_and(exists, cond),
                        here,
                        here,
                        z_send.at[direction, hop, c],
                        z_recv.at[direction, hop, c],
                        target,
                    )
                key = (1 + direction * (length - 1) + hop - 1) * count + c
                copies.start(exists, here, here, y_send.at[key], y_recv.at[key], other)
    wait_arrival(o_ref.at[other, first], y_send.at[y_first], y_recv.at[y_first], other)
    for direction in range(2):
        z_hop(direction, 0, count, x_ref.at[first], o_ref.at[me, first])
        z_hop(direction, 0, count + 1, o_ref.at[other, first], o_ref.at[other, first])
    for hop in range(1, length):
        for line, base in enumerate((me, other)):
            for direction in range(2):
                source = base - 2 * hop if direction == 0 else base + 2 * hop
                exists = source >= 0 if direction == 0 else source < n
                sender = me - 2 if direction == 0 else me + 2

                @pl.when(exists)
                def _():
                    wait_arrival(
                        o_ref.at[source, first],
                        z_send.at[direction, hop - 1, count + line],
                        z_recv.at[direction, hop - 1, count + line],
                        sender,
                    )

                here = o_ref.at[source, first]
                if hop < length - 1:
                    cond, target = nexts[direction]
                    copies.start(
                        jnp.logical_and(exists, cond),
                        here,
                        here,
                        z_send.at[direction, hop, count + line],
                        z_recv.at[direction, hop, count + line],
                        target,
                    )
    for c, (at, size) in enumerate(chunks):
        span = pl.ds(at, size)
        wait_arrival(o_ref.at[other, span], y_send.at[c], y_recv.at[c], other)
        for hop in range(1, length):
            for direction in range(2):
                source = other - 2 * hop if direction == 0 else other + 2 * hop
                exists = source >= 0 if direction == 0 else source < n
                key = (1 + direction * (length - 1) + hop - 1) * count + c

                @pl.when(exists)
                def _():
                    wait_arrival(o_ref.at[source, span], y_send.at[key], y_recv.at[key], other)

    own.wait()
    copies.finish()


def gather_rows(x):
    n = lax.axis_size("shard")
    rows, columns = x.shape
    if not use_kernels(n, rows):
        return lax.all_gather(x, "shard", axis=0, tiled=False)
    across, chunks = split_rows(rows)
    length, count = n // 2, len(chunks)
    keys = (2 * length - 1) * count + 1
    return pl.pallas_call(
        functools.partial(gather_kernel, n, across, chunks),
        out_shape=jax.ShapeDtypeStruct((n, rows, columns), x.dtype),
        in_specs=[pl.BlockSpec(memory_space=pltpu.VMEM)],
        out_specs=pl.BlockSpec(memory_space=pl.ANY),
        scratch_shapes=[
            pltpu.SemaphoreType.DMA,
            pltpu.SemaphoreType.DMA((2, length - 1, count + 2)),
            pltpu.SemaphoreType.DMA((2, length - 1, count + 2)),
            pltpu.SemaphoreType.DMA((keys,)),
            pltpu.SemaphoreType.DMA((keys,)),
        ],
        compiler_params=pltpu.CompilerParams(collective_id=1, has_side_effects=True),
        cost_estimate=wire_cost(n * rows * columns * 2),
        name="gather_rows",
    )(x)


def add_rows(*terms):
    total = terms[0].astype(jnp.float32)
    for term in terms[1:]:
        total = total + term.astype(jnp.float32)
    return total


def scatter_kernel(
    n, across, chunks, p_ref, o_ref, y_buf, z_buf, a_buf, a_got, z_send, z_recv, y_send, y_recv
):
    length = n // 2
    count = len(chunks)
    me = lax.axis_index("shard")
    place, side = me // 2, me % 2
    other = me + 1 - 2 * side
    has_left, has_right = place > 0, place < length - 1
    greet(has_left, has_right, me - 2, me + 2, other)
    copies = Copies()
    first = pl.ds(0, across)

    def routes():
        for distance in range(length - 1, 0, -1):
            yield 0, distance, place + distance, place + distance < length
            yield 1, distance, place - distance, place - distance >= 0

    behind = (has_left, has_right)
    sender = (me - 2, me + 2)
    target = (me + 2, me - 2)

    for direction, distance, owner, exists in routes():
        for c, (at, size) in enumerate(chunks):
            key = (direction * (length - 1) + distance - 1) * count + c
            copies.start(
                exists,
                p_ref.at[2 * owner + 1 - side, pl.ds(at, size)],
                y_buf.at[direction * (length - 1) + distance - 1, pl.ds(at - across, size)],
                y_send.at[key],
                y_recv.at[key],
                other,
            )
    mid = 2 * (length - 1)
    for c, (at, size) in enumerate(chunks):
        key = mid * count + c
        copies.start(
            None,
            p_ref.at[2 * place + 1 - side, pl.ds(at, size)],
            y_buf.at[mid, pl.ds(at - across, size)],
            y_send.at[key],
            y_recv.at[key],
            other,
        )

    def z_dst(direction, distance, at, size):
        return z_buf.at[direction, distance, pl.ds(at, size)]

    for direction, distance, owner, exists in routes():
        for line in range(2):
            block = 2 * owner + (side if line == 0 else 1 - side)
            sem_in = (direction, distance, count + line)
            sem_out = (direction, distance - 1, count + line)
            place_rows = line * across
            from_start = jnp.logical_and(exists, jnp.logical_not(behind[direction]))
            passing = jnp.logical_and(exists, behind[direction])
            dst = z_dst(direction, distance - 1, place_rows, across)
            copies.start(
                from_start,
                p_ref.at[block, first],
                dst,
                z_send.at[sem_out],
                z_recv.at[sem_out],
                target[direction],
            )
            if distance < length - 1:
                here = z_dst(direction, distance, place_rows, across)

                @pl.when(passing)
                def _():
                    wait_arrival(here, z_send.at[sem_in], z_recv.at[sem_in], sender[direction])
                    here[...] = add_rows(here[...], p_ref[block, first]).astype(here.dtype)

                copies.start(
                    passing, here, dst, z_send.at[sem_out], z_recv.at[sem_out], target[direction]
                )

    for line in (1, 0):
        block = 2 * place + (side if line == 0 else 1 - side)
        o_ref[first] = p_ref[block, first].astype(jnp.float32)
        for direction in range(2):
            sem_in = (direction, 0, count + line)
            here = z_dst(direction, 0, line * across, across)

            @pl.when(behind[direction])
            def _():
                wait_arrival(here, z_send.at[sem_in], z_recv.at[sem_in], sender[direction])
                o_ref[first] = o_ref[first] + here[...].astype(jnp.float32)

        if line == 1:
            a_buf[...] = o_ref[first].astype(a_buf.dtype)
            key = (mid + 1) * count
            copies.start(None, a_buf, a_got, y_send.at[key], y_recv.at[key], other)

    for direction, distance, owner, exists in routes():
        slot = direction * (length - 1) + distance - 1
        for c, (at, size) in enumerate(chunks):
            key = slot * count + c
            held = y_buf.at[slot, pl.ds(at - across, size)]
            block = 2 * owner + side
            sem_in = (direction, distance, c)
            sem_out = (direction, distance - 1, c)
            rows_at = across + at
            span = pl.ds(at, size)

            @pl.when(exists)
            def _():
                wait_arrival(held, y_send.at[key], y_recv.at[key], other)

            if distance < length - 1:
                here = z_dst(direction, distance, rows_at, size)

                @pl.when(jnp.logical_and(exists, behind[direction]))
                def _():
                    wait_arrival(here, z_send.at[sem_in], z_recv.at[sem_in], sender[direction])
                    held[...] = add_rows(held[...], p_ref[block, span], here[...]).astype(
                        held.dtype
                    )

            @pl.when(jnp.logical_and(exists, jnp.logical_not(behind[direction])))
            def _():
                held[...] = add_rows(held[...], p_ref[block, span]).astype(held.dtype)

            copies.start(
                exists,
                held,
                z_dst(direction, distance - 1, rows_at, size),
                z_send.at[sem_out],
                z_recv.at[sem_out],
                target[direction],
            )
    for c, (at, size) in enumerate(chunks):
        key = mid * count + c
        held = y_buf.at[mid, pl.ds(at - across, size)]
        span = pl.ds(at, size)
        wait_arrival(held, y_send.at[key], y_recv.at[key], other)
        o_ref[span] = add_rows(held[...], p_ref[me, span])
        for direction in range(2):
            sem_in = (direction, 0, c)
            here = z_dst(direction, 0, across + at, size)

            @pl.when(behind[direction])
            def _():
                wait_arrival(here, z_send.at[sem_in], z_recv.at[sem_in], sender[direction])
                o_ref[span] = o_ref[span] + here[...].astype(jnp.float32)

    key = (mid + 1) * count
    wait_arrival(a_got, y_send.at[key], y_recv.at[key], other)
    o_ref[first] = o_ref[first] + a_got[...].astype(jnp.float32)
    copies.finish()


def scatter_rows(partial):
    n, rows, columns = partial.shape
    if not use_kernels(n, rows):
        return lax.psum_scatter(
            partial.reshape(n * rows, columns), "shard", scatter_dimension=0, tiled=True
        ).astype(jnp.float32)
    across, chunks = split_rows(rows)
    length, count = n // 2, len(chunks)
    late = rows - across
    keys = (2 * length - 1) * count + 1
    dtype = partial.dtype
    return pl.pallas_call(
        functools.partial(scatter_kernel, n, across, chunks),
        out_shape=jax.ShapeDtypeStruct((rows, columns), jnp.float32),
        in_specs=[pl.BlockSpec(memory_space=pltpu.VMEM)],
        out_specs=pl.BlockSpec(memory_space=pltpu.VMEM),
        scratch_shapes=[
            pltpu.VMEM((2 * length - 1, late, columns), dtype),
            pltpu.VMEM((2, length - 1, across + rows, columns), dtype),
            pltpu.VMEM((across, columns), dtype),
            pltpu.VMEM((across, columns), dtype),
            pltpu.SemaphoreType.DMA((2, length - 1, count + 2)),
            pltpu.SemaphoreType.DMA((2, length - 1, count + 2)),
            pltpu.SemaphoreType.DMA((keys,)),
            pltpu.SemaphoreType.DMA((keys,)),
        ],
        compiler_params=pltpu.CompilerParams(collective_id=2, has_side_effects=True),
        cost_estimate=wire_cost(n * rows * columns * 2),
        name="scatter_rows",
    )(partial)


def small_gather_kernel(n, a_ref, b_ref, a_out, b_out, send, recv):
    me = lax.axis_index("shard")
    barrier = pltpu.get_barrier_semaphore()
    peers = [lax.rem(me + d, n) for d in range(1, n)]
    for peer in peers:
        pl.semaphore_signal(barrier, inc=1, device_id={"shard": peer}, device_id_type=MESH)
    pl.semaphore_wait(barrier, n - 1)
    copies = Copies()
    for d, peer in enumerate(peers):
        for k, (src, dst) in enumerate(((a_ref, a_out), (b_ref, b_out))):
            copies.start(None, src, dst.at[me], send.at[k, d], recv.at[k, d], peer)
    a_out[me] = a_ref[...]
    b_out[me] = b_ref[...]
    for d in range(1, n):
        source = lax.rem(me + n - d, n)
        for k, dst in enumerate((a_out, b_out)):
            wait_arrival(dst.at[source], send.at[k, d - 1], recv.at[k, d - 1], source)
    copies.finish()


def gather_small(gains, segment_ids):
    n = lax.axis_size("shard")
    width, length = gains.shape[1], segment_ids.shape[1]
    if not use_kernels(n, 256) or width % 128 or length % 128:
        gains = lax.all_gather(gains, "shard", axis=1, tiled=True)
        return gains, lax.all_gather(segment_ids, "shard", axis=0, tiled=True)
    gains = jnp.pad(gains.astype(jnp.float32), ((0, 6), (0, 0)))
    ids = jnp.broadcast_to(segment_ids, (8, length))
    all_gains, all_ids = pl.pallas_call(
        functools.partial(small_gather_kernel, n),
        out_shape=(
            jax.ShapeDtypeStruct((n, 8, width), jnp.float32),
            jax.ShapeDtypeStruct((n, 8, length), jnp.int32),
        ),
        in_specs=[pl.BlockSpec(memory_space=pltpu.VMEM)] * 2,
        out_specs=[pl.BlockSpec(memory_space=pltpu.VMEM)] * 2,
        scratch_shapes=[pltpu.SemaphoreType.DMA((2, n - 1)), pltpu.SemaphoreType.DMA((2, n - 1))],
        compiler_params=pltpu.CompilerParams(collective_id=3, has_side_effects=True),
        name="gather_small",
    )(gains, ids)
    return all_gains[:, :2].transpose(1, 0, 2).reshape(2, n * width), all_ids[:, 0]


def small_sum_kernel(n, m, t_ref, o_ref, got, mine, shared, send, recv, send_two, recv_two):
    me, copy = lax.axis_index("shard"), lax.axis_index("replica")
    barrier = pltpu.get_barrier_semaphore()
    peers = [lax.rem(me + d, n) for d in range(1, n)]
    twins = [lax.rem(copy + d, m) for d in range(1, m)]
    for peer in peers:
        pl.semaphore_signal(barrier, inc=1, device_id={"shard": peer}, device_id_type=MESH)
    for twin in twins:
        pl.semaphore_signal(barrier, inc=1, device_id={"replica": twin}, device_id_type=MESH)
    pl.semaphore_wait(barrier, n + m - 2)
    copies = Copies()
    for d, peer in enumerate(peers):
        copies.start(None, t_ref.at[peer], got.at[me], send.at[d], recv.at[d], peer)
    got[me] = t_ref[me]
    for d in range(1, n):
        source = lax.rem(me + n - d, n)
        wait_arrival(got.at[source], send.at[d - 1], recv.at[d - 1], source)
    total = got[0]
    for i in range(1, n):
        total = total + got[i]
    mine[...] = total
    shared[copy] = total
    for d, twin in enumerate(twins):
        copies.start(
            None, mine, shared.at[copy], send_two.at[d], recv_two.at[d], twin, axis="replica"
        )
    for d in range(1, m):
        source = lax.rem(copy + m - d, m)
        wait_arrival(
            shared.at[source], send_two.at[d - 1], recv_two.at[d - 1], source, axis="replica"
        )
    total = shared[0]
    for i in range(1, m):
        total = total + shared[i]
    o_ref[...] = total
    copies.finish()


def sum_small(terms):
    n, m = lax.axis_size("shard"), lax.axis_size("replica")
    width = terms.shape[1] // n
    if not use_kernels(n, 256) or width % 128:
        total = lax.psum(terms, ("replica", "shard"))
        return lax.dynamic_slice_in_dim(total, lax.axis_index("shard") * width, width, axis=1)
    pieces = jnp.pad(terms, ((0, 6), (0, 0))).reshape(8, n, width).transpose(1, 0, 2)
    return pl.pallas_call(
        functools.partial(small_sum_kernel, n, m),
        out_shape=jax.ShapeDtypeStruct((8, width), jnp.float32),
        in_specs=[pl.BlockSpec(memory_space=pltpu.VMEM)],
        out_specs=pl.BlockSpec(memory_space=pltpu.VMEM),
        scratch_shapes=[
            pltpu.VMEM((n, 8, width), jnp.float32),
            pltpu.VMEM((8, width), jnp.float32),
            pltpu.VMEM((m, 8, width), jnp.float32),
            pltpu.SemaphoreType.DMA((n - 1,)),
            pltpu.SemaphoreType.DMA((n - 1,)),
            pltpu.SemaphoreType.DMA((m - 1,)),
            pltpu.SemaphoreType.DMA((m - 1,)),
        ],
        compiler_params=pltpu.CompilerParams(collective_id=4, has_side_effects=True),
        name="sum_small",
    )(pieces)[:2]


def after(x, *others):
    return lax.optimization_barrier((x,) + others)[0]


def to_columns(weights):
    n, copies = lax.axis_size("shard"), lax.axis_size("replica")
    me = lax.axis_index("replica")
    rows = weights[0].shape[0]
    part = rows // copies
    pieces = [
        lax.dynamic_slice_in_dim(w, me * part, part).reshape(part, n, -1).transpose(1, 0, 2)
        for w in weights
    ]
    swapped = lax.all_to_all(
        jnp.concatenate(pieces, axis=2), "shard", split_axis=0, concat_axis=0, tiled=True
    )
    shared = lax.all_gather(swapped, "replica", axis=1, tiled=False)
    return shared.reshape(n * rows, -1)


def sum_copies(grads):
    n, copies = lax.axis_size("shard"), lax.axis_size("replica")
    rows, width = grads.shape[0] // n, grads.shape[1]
    split = grads.reshape(n, copies, rows // copies, width).transpose(1, 0, 2, 3)
    return lax.psum_scatter(split, "replica", scatter_dimension=0, tiled=False)


def unpack_kernel(widths, x_ref, *o_refs):
    copies, _, part, _ = x_ref.shape
    at = 0
    for width, o_ref in zip(widths, o_refs):
        for r in range(copies):
            o_ref[pl.ds(r * part, part)] = x_ref[r, 0, :, pl.ds(at, width)].astype(o_ref.dtype)
        at += width


def to_rows(summed, widths):
    swapped = lax.all_to_all(summed, "shard", split_axis=0, concat_axis=0, tiled=True)
    return unpack(lax.all_gather(swapped, "replica", axis=0, tiled=False), widths)


def unpack(shared, widths):
    copies, n, part, total = shared.shape
    rows = copies * part
    if part % 16 == 0 and all(width % 128 == 0 for width in widths):
        return pl.pallas_call(
            functools.partial(unpack_kernel, widths),
            grid=(n,),
            out_shape=[jax.ShapeDtypeStruct((rows, n * width), jnp.float32) for width in widths],
            in_specs=[pl.BlockSpec((copies, 1, part, total), lambda i: (0, i, 0, 0))],
            out_specs=[pl.BlockSpec((rows, width), lambda i: (0, i)) for width in widths],
            name="unpack",
        )(shared)
    out, at = [], 0
    for width in widths:
        piece = shared[..., at : at + width].transpose(0, 2, 1, 3).reshape(rows, n * width)
        out.append(piece.astype(jnp.float32))
        at += width
    return out


def positions_tables(segment_rows, head_dim):
    length_all = segment_rows.shape[1]
    counter = lax.broadcasted_iota(jnp.int32, segment_rows.shape, 1)
    is_first = jnp.concatenate(
        [
            jnp.ones((segment_rows.shape[0], 1), jnp.bool_),
            segment_rows[:, 1:] != segment_rows[:, :-1],
        ],
        axis=1,
    )
    first_at = lax.cummax(jnp.where(is_first, counter, jnp.zeros_like(counter)), axis=1)
    position = (counter - first_at).astype(jnp.float32).reshape(-1)
    half_dim = head_dim // 2
    inverse = jnp.exp(
        -(jnp.arange(half_dim, dtype=jnp.float32) * (2.0 / head_dim)) * math.log(THETA)
    )
    angles = position[:, None] * inverse[None, :]
    return (jnp.cos(angles), jnp.sin(angles))


def rotate(values, cosine, sine_tab, direction, head_dim):
    row_count, total_width = values.shape
    half_dim = head_dim // 2
    halves = values.reshape(row_count, total_width // head_dim, 2, half_dim)
    first_half = halves[:, :, 0]
    second_half = halves[:, :, 1]
    cos_wide = cosine[:, None, :]
    sin_wide = direction * sine_tab[:, None, :]
    turned = jnp.stack(
        [
            first_half * cos_wide - second_half * sin_wide,
            second_half * cos_wide + first_half * sin_wide,
        ],
        axis=2,
    )
    return turned.reshape(row_count, total_width)


def allowed(segment_rows):
    ids = jnp.arange(segment_rows.shape[1], dtype=jnp.int32)
    return (segment_rows[:, :, None] == segment_rows[:, None, :]) & (
        ids[None, None, :] <= ids[None, :, None]
    )


def heads_of(values, packs, head_dim):
    return values.reshape(packs, values.shape[0] // packs, -1, head_dim)


def pair_scores(q_heads, k_heads, mask):
    scores = (
        jnp.einsum("pqhd,pkhd->phqk", q_heads, k_heads, preferred_element_type=jnp.float32) * SCALE
    )
    return jnp.where(mask[:, None], scores, -1e30)


def attention_forward(q_rot, k_rot, v_vals, segment_rows, head_dim):
    packs = segment_rows.shape[0]
    q_heads, k_heads, v_heads = (heads_of(v, packs, head_dim) for v in (q_rot, k_rot, v_vals))
    scores = pair_scores(q_heads, k_heads, allowed(segment_rows))
    log_total = jnp.log(jnp.sum(jnp.exp(scores), axis=-1))
    rounded_probs = jnp.exp(scores - log_total[..., None]).astype(jnp.bfloat16)
    mixed_out = jnp.einsum(
        "phqk,pkhd->pqhd", rounded_probs, v_heads, preferred_element_type=jnp.float32
    )
    return mixed_out.astype(jnp.bfloat16).reshape(q_rot.shape), log_total


def attention_backward(q_rot, k_rot, v_vals, log_total, grad_att, segment_rows, head_dim):
    packs = segment_rows.shape[0]
    q_heads, k_heads, v_heads, g_heads = (
        heads_of(v, packs, head_dim) for v in (q_rot, k_rot, v_vals, grad_att)
    )
    scores = pair_scores(q_heads, k_heads, allowed(segment_rows))
    attn_probs = jnp.exp(scores - log_total[..., None])
    grad_probs = jnp.einsum("pqhd,pkhd->phqk", g_heads, v_heads, preferred_element_type=jnp.float32)
    inner_sum = jnp.sum(attn_probs * grad_probs, axis=-1, keepdims=True)
    grad_scores = (attn_probs * (grad_probs - inner_sum) * SCALE).astype(jnp.bfloat16)
    rounded_probs = attn_probs.astype(jnp.bfloat16)
    grad_q = jnp.einsum("phqk,pkhd->pqhd", grad_scores, k_heads, preferred_element_type=jnp.float32)
    grad_k = jnp.einsum("phqk,pqhd->pkhd", grad_scores, q_heads, preferred_element_type=jnp.float32)
    grad_v = jnp.einsum(
        "phqk,pqhd->pkhd", rounded_probs, g_heads, preferred_element_type=jnp.float32
    )
    return tuple(g.reshape(q_rot.shape) for g in (grad_q, grad_k, grad_v))


def turn(values, cosine, sine_tab, direction):
    lane = lax.broadcasted_iota(jnp.int32, values.shape, 1)
    is_first = lane % HEAD_DIM < HEAD_DIM // 2
    width = values.shape[1]
    swapped = jnp.where(
        is_first,
        pltpu.roll(values, width - HEAD_DIM // 2, 1),
        pltpu.roll(values, HEAD_DIM // 2, 1),
    )
    return values * cosine + swapped * jnp.where(is_first, -direction, direction) * sine_tab


def head_probs(q_head, k_head, mask):
    scores = jnp.where(mask, times_transposed(q_head, k_head) * SCALE, -1e30)
    log_total = jnp.log(jnp.sum(jnp.exp(scores), axis=-1, keepdims=True))
    return jnp.exp(scores - log_total)


def attend_kernel(width, qkv_ref, cos_ref, sin_ref, mask_ref, rot_ref, att_ref):
    cosine, sine_tab = cos_ref[...], sin_ref[...]
    mask = mask_ref[0] > 0.5
    lanes = 2 * HEAD_DIM
    for at in range(0, width, lanes):
        q_two = turn(qkv_ref[:, at : at + lanes], cosine, sine_tab, 1.0).astype(jnp.bfloat16)
        k_at, v_at = width + at, 2 * width + at
        k_two = turn(qkv_ref[:, k_at : k_at + lanes], cosine, sine_tab, 1.0).astype(jnp.bfloat16)
        v_two = qkv_ref[:, v_at : v_at + lanes].astype(jnp.bfloat16)
        rot_ref[:, at : at + lanes] = q_two
        rot_ref[:, k_at : k_at + lanes] = k_two
        rot_ref[:, v_at : v_at + lanes] = v_two
        mixed = []
        for h in range(0, lanes, HEAD_DIM):
            one = slice(h, h + HEAD_DIM)
            probs = head_probs(q_two[:, one], k_two[:, one], mask).astype(jnp.bfloat16)
            mixed.append(times_plain(probs, v_two[:, one]))
        att_ref[:, at : at + lanes] = jnp.concatenate(mixed, axis=1).astype(att_ref.dtype)


def attend_back_kernel(width, rot_ref, g_ref, cos_ref, sin_ref, mask_ref, back_ref):
    cosine, sine_tab = cos_ref[...], sin_ref[...]
    mask = mask_ref[0] > 0.5
    lanes = 2 * HEAD_DIM
    for at in range(0, width, lanes):
        k_at, v_at = width + at, 2 * width + at
        q_two = rot_ref[:, at : at + lanes]
        k_two = rot_ref[:, k_at : k_at + lanes]
        v_two = rot_ref[:, v_at : v_at + lanes]
        g_two = g_ref[:, at : at + lanes]
        grads = ([], [], [])
        for h in range(0, lanes, HEAD_DIM):
            one = slice(h, h + HEAD_DIM)
            q, k, v, g = q_two[:, one], k_two[:, one], v_two[:, one], g_two[:, one]
            probs = head_probs(q, k, mask)
            grad_probs = times_transposed(g, v)
            inner = jnp.sum(probs * grad_probs, axis=-1, keepdims=True)
            grad_scores = (probs * (grad_probs - inner) * SCALE).astype(jnp.bfloat16)
            grads[0].append(times_plain(grad_scores, k))
            grads[1].append(token_contract(grad_scores, q))
            grads[2].append(token_contract(probs.astype(jnp.bfloat16), g))
        grad_q, grad_k, grad_v = (jnp.concatenate(g, axis=1) for g in grads)
        dtype = back_ref.dtype
        back_ref[:, at : at + lanes] = turn(grad_q, cosine, sine_tab, -1.0).astype(dtype)
        back_ref[:, k_at : k_at + lanes] = turn(grad_k, cosine, sine_tab, -1.0).astype(dtype)
        back_ref[:, v_at : v_at + lanes] = grad_v.astype(dtype)


def pack_specs(length, *widths):
    return [pl.BlockSpec((length, width), lambda i: (i, 0)) for width in widths]


def wide_tables(segment_rows):
    cosine, sine_tab = positions_tables(segment_rows, HEAD_DIM)
    mask = allowed(segment_rows).astype(jnp.float32)
    return jnp.tile(cosine, (1, 4)), jnp.tile(sine_tab, (1, 4)), mask


def attend(qkv, tables):
    cosine, sine_tab, mask = tables
    packs, length, _ = mask.shape
    tokens, width = qkv.shape[0], qkv.shape[1] // 3
    return pl.pallas_call(
        functools.partial(attend_kernel, width),
        grid=(packs,),
        out_shape=[
            jax.ShapeDtypeStruct((tokens, 3 * width), jnp.bfloat16),
            jax.ShapeDtypeStruct((tokens, width), jnp.bfloat16),
        ],
        in_specs=pack_specs(length, 3 * width, 2 * HEAD_DIM, 2 * HEAD_DIM)
        + [pl.BlockSpec((1, length, length), lambda i: (i, 0, 0))],
        out_specs=pack_specs(length, 3 * width, width),
        name="attend",
    )(qkv, cosine, sine_tab, mask)


def attend_back(rotated, grad_att, tables):
    cosine, sine_tab, mask = tables
    packs, length, _ = mask.shape
    tokens, width = grad_att.shape
    return pl.pallas_call(
        functools.partial(attend_back_kernel, width),
        grid=(packs,),
        out_shape=jax.ShapeDtypeStruct((tokens, 3 * width), jnp.bfloat16),
        in_specs=pack_specs(length, 3 * width, width, 2 * HEAD_DIM, 2 * HEAD_DIM)
        + [pl.BlockSpec((1, length, length), lambda i: (i, 0, 0))],
        out_specs=pack_specs(length, 3 * width)[0],
        name="attend_back",
    )(rotated, grad_att, cosine, sine_tab, mask)


def attend_plain(qkv, segment_rows):
    width = qkv.shape[1] // 3
    cosine, sine_tab = positions_tables(segment_rows, HEAD_DIM)
    q_rot = rotate(qkv[:, :width], cosine, sine_tab, 1.0, HEAD_DIM).astype(jnp.bfloat16)
    k_rot = rotate(qkv[:, width : 2 * width], cosine, sine_tab, 1.0, HEAD_DIM).astype(jnp.bfloat16)
    v_vals = qkv[:, 2 * width :].astype(jnp.bfloat16)
    attended, log_total = attention_forward(q_rot, k_rot, v_vals, segment_rows, HEAD_DIM)
    return (q_rot, k_rot, v_vals, log_total), attended


def attend_back_plain(rotated, grad_att, segment_rows):
    cosine, sine_tab = positions_tables(segment_rows, HEAD_DIM)
    q_rot, k_rot, v_vals, log_total = rotated
    grad_q, grad_k, grad_v = attention_backward(
        q_rot, k_rot, v_vals, log_total, grad_att, segment_rows, HEAD_DIM
    )
    q_back = rotate(grad_q, cosine, sine_tab, -1.0, HEAD_DIM)
    k_back = rotate(grad_k, cosine, sine_tab, -1.0, HEAD_DIM)
    return jnp.concatenate([q_back, k_back, grad_v], axis=1).astype(jnp.bfloat16)


def norm_scale(values):
    return lax.rsqrt(jnp.mean(values * values, axis=-1, keepdims=True) + EPS)


def norm_back(upstream, source, scale, gain, grad_normed):
    gain_term = jnp.sum(grad_normed * source * scale, axis=0)
    weighted = gain * grad_normed
    grad = (
        upstream
        + scale * weighted
        - source * (scale * scale * scale) * jnp.mean(weighted * source, axis=-1, keepdims=True)
    )
    return grad, gain_term


def per_device(
    block_input,
    segment_ids,
    attn_gain,
    mlp_gain,
    w_query,
    w_key,
    w_value,
    w_out,
    w_gate,
    w_up,
    w_down,
    out_grad,
):
    n = lax.axis_size("shard")
    row_count, model_width = block_input.shape

    def spread(x):
        return gather_rows(x).reshape(n * row_count, -1)

    def collect(partial):
        return scatter_rows(partial.astype(jnp.bfloat16).reshape(n, row_count, model_width))

    gains, segment_rows = gather_small(jnp.stack([attn_gain, mlp_gain]), segment_ids)
    gain_one, gain_two = gains[0].astype(jnp.float32), gains[1].astype(jnp.float32)
    qkv_cols = to_columns((w_query, w_key, w_value))
    pair_cols = to_columns((w_gate, w_up))
    head_width, ff_width = qkv_cols.shape[1] // 3, pair_cols.shape[1] // 2
    gate_cols, up_cols = pair_cols[:, :ff_width], pair_cols[:, ff_width:]
    by_kernel = head_width % (2 * HEAD_DIM) == 0

    input_f = block_input.astype(jnp.float32)
    scale_one = norm_scale(input_f)
    normed_one = spread((input_f * scale_one * gain_one).astype(jnp.bfloat16))
    cotangent = lax.all_gather(after(out_grad, normed_one), "shard", axis=0, tiled=True)
    qkv = times_plain(normed_one, qkv_cols)
    if by_kernel:
        tables = wide_tables(segment_rows)
        rotated, attended = attend(qkv, tables)
    else:
        rotated, attended = attend_plain(qkv, segment_rows)
    residual = input_f + collect(times_plain(attended, w_out))
    scale_two = norm_scale(residual)
    normed_two = spread((residual * scale_two * gain_two).astype(jnp.bfloat16))
    gate_pre = times_plain(normed_two, gate_cols)
    up_pre = times_plain(normed_two, up_cols)
    gate_sig = jax.nn.sigmoid(gate_pre)
    silu_val = gate_pre * gate_sig
    hidden_b = (silu_val * up_pre).astype(jnp.bfloat16)
    block_output = (residual + collect(times_plain(hidden_b, w_down))).astype(jnp.bfloat16)

    grad_hidden = times_transposed(cotangent, w_down)
    gate_b = (grad_hidden * up_pre * gate_sig * (1.0 + gate_pre * (1.0 - gate_sig))).astype(
        jnp.bfloat16
    )
    up_b = (grad_hidden * silu_val).astype(jnp.bfloat16)
    pair_b = jnp.concatenate([gate_b, up_b], axis=1)
    pair_sum = sum_copies(token_contract(normed_two, pair_b).astype(jnp.bfloat16))
    grad_down = token_contract(hidden_b, cotangent).astype(jnp.bfloat16)
    grad_down = lax.psum(after(grad_down, pair_sum), "replica")
    grad_normed_two = collect(times_transposed(pair_b, pair_cols))
    grad_residual, gain_two_term = norm_back(
        out_grad.astype(jnp.float32), residual, scale_two, gain_two, grad_normed_two
    )
    residual_b = spread(grad_residual.astype(jnp.bfloat16))
    grad_gate, grad_up = to_rows(after(pair_sum, residual_b), (ff_width, ff_width))
    grad_out = token_contract(attended, residual_b).astype(jnp.bfloat16)
    grad_out = lax.psum(after(grad_out, grad_down), "replica")
    grad_att = times_transposed(residual_b, w_out).astype(jnp.bfloat16)
    if by_kernel:
        back = attend_back(rotated, grad_att, tables)
    else:
        back = attend_back_plain(rotated, grad_att, segment_rows)
    qkv_sum = sum_copies(
        after(token_contract(normed_one, back).astype(jnp.bfloat16), grad_out)
    )
    grad_normed_one = collect(times_transposed(back, qkv_cols))
    input_grad, gain_one_term = norm_back(
        grad_residual, input_f, scale_one, gain_one, grad_normed_one
    )
    gain_rows = sum_small(jnp.stack([gain_one_term, gain_two_term]))
    grad_query, grad_key, grad_value = to_rows(
        after(qkv_sum, grad_normed_one), (head_width,) * 3
    )
    return (
        block_output,
        input_grad,
        grad_query,
        grad_key,
        grad_value,
        grad_out.astype(jnp.float32),
        grad_gate,
        grad_up,
        grad_down.astype(jnp.float32),
        gain_rows[0],
        gain_rows[1],
    )


def solution(mesh):
    placed = (
        P(("replica", "shard"), None),
        P(("replica", "shard"), None),
        P("shard"),
        P("shard"),
        P("shard", None),
        P("shard", None),
        P("shard", None),
        P("shard", None),
        P("shard", None),
        P("shard", None),
        P("shard", None),
        P(("replica", "shard"), None),
    )
    return jax.shard_map(
        per_device,
        mesh=mesh,
        in_specs=placed,
        out_specs=(
            P(("replica", "shard"), None),
            P(("replica", "shard"), None),
            P("shard", None),
            P("shard", None),
            P("shard", None),
            P("shard", None),
            P("shard", None),
            P("shard", None),
            P("shard", None),
            P("shard"),
            P("shard"),
        ),
        check_vma=False,
    )
```

```python
import functools
import math

import jax
import jax.numpy as jnp
from jax import lax
from jax.experimental import pallas as pl
from jax.experimental.pallas import tpu as pltpu
from jax.sharding import PartitionSpec as P

MESH = pl.DeviceIdType.MESH

HEAD_DIM = 64


EPS = 1e-05
THETA = 130000.0
SCALE = 0.125


def times_plain(left_op, right_op):
    return jnp.dot(left_op, right_op, preferred_element_type=jnp.float32)


def times_transposed(left_op, right_op):
    return lax.dot_general(
        left_op, right_op, (((1,), (1,)), ((), ())), preferred_element_type=jnp.float32
    )


def token_contract(left_op, right_op):
    return lax.dot_general(
        left_op, right_op, (((0,), (0,)), ((), ())), preferred_element_type=jnp.float32
    )


def split_rows(rows):
    unit = 16
    across = (rows // unit) * 3 // 16 * unit
    rest = (rows - across) // unit
    count = min(4, rest)
    sizes = [(rest // count + (1 if i >= count - rest % count else 0)) * unit for i in range(count)]
    chunks, at = [], across
    for size in sizes:
        chunks.append((at, size))
        at += size
    return across, chunks


def use_kernels(n, rows):
    return n % 2 == 0 and 2 < n <= 8 and rows % 256 == 0


def wire_cost(size):
    return pl.CostEstimate(flops=0, bytes_accessed=30 * size, transcendentals=0)


class Copies:
    def __init__(self):
        self.started = []

    def start(self, cond, src, dst, send_sem, recv_sem, target, axis="shard"):
        copy = pltpu.make_async_remote_copy(
            src_ref=src,
            dst_ref=dst,
            send_sem=send_sem,
            recv_sem=recv_sem,
            device_id={axis: target},
            device_id_type=MESH,
        )
        if cond is None:
            copy.start()
        else:
            pl.when(cond)(copy.start)
        self.started.append((cond, copy))

    def finish(self):
        for cond, copy in self.started:
            if cond is None:
                copy.wait_send()
            else:
                pl.when(cond)(copy.wait_send)


def wait_arrival(dst, send_sem, recv_sem, source, axis="shard"):
    pltpu.make_async_remote_copy(
        src_ref=dst,
        dst_ref=dst,
        send_sem=send_sem,
        recv_sem=recv_sem,
        device_id={axis: source},
        device_id_type=MESH,
    ).wait_recv()


def greet(has_left, has_right, left, right, other):
    barrier = pltpu.get_barrier_semaphore()
    pl.semaphore_signal(barrier, inc=1, device_id={"shard": other}, device_id_type=MESH)

    @pl.when(has_left)
    def _():
        pl.semaphore_signal(barrier, inc=1, device_id={"shard": left}, device_id_type=MESH)

    @pl.when(has_right)
    def _():
        pl.semaphore_signal(barrier, inc=1, device_id={"shard": right}, device_id_type=MESH)

    pl.semaphore_wait(barrier, 1 + has_left.astype(jnp.int32) + has_right.astype(jnp.int32))


def gather_kernel(n, across, chunks, x_ref, o_ref, own_sem, z_send, z_recv, y_send, y_recv):
    length = n // 2
    count = len(chunks)
    me = lax.axis_index("shard")
    place, side = me // 2, me % 2
    other = me + 1 - 2 * side
    has_left, has_right = place > 0, place < length - 1
    nexts = ((has_right, me + 2), (has_left, me - 2))
    greet(has_left, has_right, me - 2, me + 2, other)
    copies = Copies()
    own = pltpu.make_async_copy(x_ref, o_ref.at[me], own_sem)
    own.start()
    first = pl.ds(0, across)
    y_first = (2 * length - 1) * count
    copies.start(
        None, x_ref.at[first], o_ref.at[me, first], y_send.at[y_first], y_recv.at[y_first], other
    )

    def z_hop(direction, hop, slot, src, dst):
        cond, target = nexts[direction]
        copies.start(
            cond,
            src,
            dst,
            z_send.at[direction, hop, slot],
            z_recv.at[direction, hop, slot],
            target,
        )

    def y_hop(origin, chunk, src, dst, cond, key):
        copies.start(cond, src, dst, y_send.at[key], y_recv.at[key], other)

    for c, (at, size) in enumerate(chunks):
        span = pl.ds(at, size)
        for direction in range(2):
            z_hop(direction, 0, c, x_ref.at[span], o_ref.at[me, span])
        y_hop(me, c, x_ref.at[span], o_ref.at[me, span], None, c)
    for hop in range(1, length):
        for c, (at, size) in enumerate(chunks):
            span = pl.ds(at, size)
            for direction in range(2):
                source = me - 2 * hop if direction == 0 else me + 2 * hop
                exists = source >= 0 if direction == 0 else source < n
                sender = me - 2 if direction == 0 else me + 2

                @pl.when(exists)
                def _():
                    wait_arrival(
                        o_ref.at[source, span],
                        z_send.at[direction, hop - 1, c],
                        z_recv.at[direction, hop - 1, c],
                        sender,
                    )

                here = o_ref.at[source, span]
                if hop < length - 1:
                    cond, target = nexts[direction]
                    copies.start(
                        jnp.logical_and(exists, cond),
                        here,
                        here,
                        z_send.at[direction, hop, c],
                        z_recv.at[direction, hop, c],
                        target,
                    )
                key = (1 + direction * (length - 1) + hop - 1) * count + c
                copies.start(exists, here, here, y_send.at[key], y_recv.at[key], other)
    wait_arrival(o_ref.at[other, first], y_send.at[y_first], y_recv.at[y_first], other)
    for direction in range(2):
        z_hop(direction, 0, count, x_ref.at[first], o_ref.at[me, first])
        z_hop(direction, 0, count + 1, o_ref.at[other, first], o_ref.at[other, first])
    for hop in range(1, length):
        for line, base in enumerate((me, other)):
            for direction in range(2):
                source = base - 2 * hop if direction == 0 else base + 2 * hop
                exists = source >= 0 if direction == 0 else source < n
                sender = me - 2 if direction == 0 else me + 2

                @pl.when(exists)
                def _():
                    wait_arrival(
                        o_ref.at[source, first],
                        z_send.at[direction, hop - 1, count + line],
                        z_recv.at[direction, hop - 1, count + line],
                        sender,
                    )

                here = o_ref.at[source, first]
                if hop < length - 1:
                    cond, target = nexts[direction]
                    copies.start(
                        jnp.logical_and(exists, cond),
                        here,
                        here,
                        z_send.at[direction, hop, count + line],
                        z_recv.at[direction, hop, count + line],
                        target,
                    )
    for c, (at, size) in enumerate(chunks):
        span = pl.ds(at, size)
        wait_arrival(o_ref.at[other, span], y_send.at[c], y_recv.at[c], other)
        for hop in range(1, length):
            for direction in range(2):
                source = other - 2 * hop if direction == 0 else other + 2 * hop
                exists = source >= 0 if direction == 0 else source < n
                key = (1 + direction * (length - 1) + hop - 1) * count + c

                @pl.when(exists)
                def _():
                    wait_arrival(o_ref.at[source, span], y_send.at[key], y_recv.at[key], other)

    own.wait()
    copies.finish()


def gather_rows(x, parts=1):
    n = lax.axis_size("shard")
    rows, columns = x.shape
    if not use_kernels(n, rows):
        return lax.all_gather(x, "shard", axis=0, tiled=False)
    across, chunks = split_rows(rows)
    length, count = n // 2, len(chunks)
    keys = (2 * length - 1) * count + 1
    return pl.pallas_call(
        functools.partial(gather_kernel, n, across, chunks),
        out_shape=jax.ShapeDtypeStruct((n, rows, columns), x.dtype),
        in_specs=[pl.BlockSpec(memory_space=pltpu.VMEM)],
        out_specs=pl.BlockSpec(memory_space=pl.ANY),
        scratch_shapes=[
            pltpu.SemaphoreType.DMA,
            pltpu.SemaphoreType.DMA((2, length - 1, count + 2)),
            pltpu.SemaphoreType.DMA((2, length - 1, count + 2)),
            pltpu.SemaphoreType.DMA((keys,)),
            pltpu.SemaphoreType.DMA((keys,)),
        ],
        compiler_params=pltpu.CompilerParams(collective_id=5 + parts, has_side_effects=True),
        cost_estimate=wire_cost(n * rows * columns * 2),
        name="gather_rows",
    )(x)


def add_rows(*terms):
    total = terms[0].astype(jnp.float32)
    for term in terms[1:]:
        total = total + term.astype(jnp.float32)
    return total


def scatter_kernel(
    n, across, chunks, p_ref, o_ref, y_buf, z_buf, a_buf, a_got, z_send, z_recv, y_send, y_recv
):
    length = n // 2
    count = len(chunks)
    me = lax.axis_index("shard")
    place, side = me // 2, me % 2
    other = me + 1 - 2 * side
    has_left, has_right = place > 0, place < length - 1
    greet(has_left, has_right, me - 2, me + 2, other)
    copies = Copies()
    first = pl.ds(0, across)

    def routes():
        for distance in range(length - 1, 0, -1):
            yield 0, distance, place + distance, place + distance < length
            yield 1, distance, place - distance, place - distance >= 0

    behind = (has_left, has_right)
    sender = (me - 2, me + 2)
    target = (me + 2, me - 2)

    for direction, distance, owner, exists in routes():
        for c, (at, size) in enumerate(chunks):
            key = (direction * (length - 1) + distance - 1) * count + c
            copies.start(
                exists,
                p_ref.at[2 * owner + 1 - side, pl.ds(at, size)],
                y_buf.at[direction * (length - 1) + distance - 1, pl.ds(at - across, size)],
                y_send.at[key],
                y_recv.at[key],
                other,
            )
    mid = 2 * (length - 1)
    for c, (at, size) in enumerate(chunks):
        key = mid * count + c
        copies.start(
            None,
            p_ref.at[2 * place + 1 - side, pl.ds(at, size)],
            y_buf.at[mid, pl.ds(at - across, size)],
            y_send.at[key],
            y_recv.at[key],
            other,
        )

    def z_dst(direction, distance, at, size):
        return z_buf.at[direction, distance, pl.ds(at, size)]

    for direction, distance, owner, exists in routes():
        for line in range(2):
            block = 2 * owner + (side if line == 0 else 1 - side)
            sem_in = (direction, distance, count + line)
            sem_out = (direction, distance - 1, count + line)
            place_rows = line * across
            from_start = jnp.logical_and(exists, jnp.logical_not(behind[direction]))
            passing = jnp.logical_and(exists, behind[direction])
            dst = z_dst(direction, distance - 1, place_rows, across)
            copies.start(
                from_start,
                p_ref.at[block, first],
                dst,
                z_send.at[sem_out],
                z_recv.at[sem_out],
                target[direction],
            )
            if distance < length - 1:
                here = z_dst(direction, distance, place_rows, across)

                @pl.when(passing)
                def _():
                    wait_arrival(here, z_send.at[sem_in], z_recv.at[sem_in], sender[direction])
                    here[...] = add_rows(here[...], p_ref[block, first]).astype(here.dtype)

                copies.start(
                    passing, here, dst, z_send.at[sem_out], z_recv.at[sem_out], target[direction]
                )

    for line in (1, 0):
        block = 2 * place + (side if line == 0 else 1 - side)
        o_ref[first] = p_ref[block, first].astype(jnp.float32)
        for direction in range(2):
            sem_in = (direction, 0, count + line)
            here = z_dst(direction, 0, line * across, across)

            @pl.when(behind[direction])
            def _():
                wait_arrival(here, z_send.at[sem_in], z_recv.at[sem_in], sender[direction])
                o_ref[first] = o_ref[first] + here[...].astype(jnp.float32)

        if line == 1:
            a_buf[...] = o_ref[first].astype(a_buf.dtype)
            key = (mid + 1) * count
            copies.start(None, a_buf, a_got, y_send.at[key], y_recv.at[key], other)

    for direction, distance, owner, exists in routes():
        slot = direction * (length - 1) + distance - 1
        for c, (at, size) in enumerate(chunks):
            key = slot * count + c
            held = y_buf.at[slot, pl.ds(at - across, size)]
            block = 2 * owner + side
            sem_in = (direction, distance, c)
            sem_out = (direction, distance - 1, c)
            rows_at = across + at
            span = pl.ds(at, size)

            @pl.when(exists)
            def _():
                wait_arrival(held, y_send.at[key], y_recv.at[key], other)

            if distance < length - 1:
                here = z_dst(direction, distance, rows_at, size)

                @pl.when(jnp.logical_and(exists, behind[direction]))
                def _():
                    wait_arrival(here, z_send.at[sem_in], z_recv.at[sem_in], sender[direction])
                    held[...] = add_rows(held[...], p_ref[block, span], here[...]).astype(
                        held.dtype
                    )

            @pl.when(jnp.logical_and(exists, jnp.logical_not(behind[direction])))
            def _():
                held[...] = add_rows(held[...], p_ref[block, span]).astype(held.dtype)

            copies.start(
                exists,
                held,
                z_dst(direction, distance - 1, rows_at, size),
                z_send.at[sem_out],
                z_recv.at[sem_out],
                target[direction],
            )
    for c, (at, size) in enumerate(chunks):
        key = mid * count + c
        held = y_buf.at[mid, pl.ds(at - across, size)]
        span = pl.ds(at, size)
        wait_arrival(held, y_send.at[key], y_recv.at[key], other)
        o_ref[span] = add_rows(held[...], p_ref[me, span])
        for direction in range(2):
            sem_in = (direction, 0, c)
            here = z_dst(direction, 0, across + at, size)

            @pl.when(behind[direction])
            def _():
                wait_arrival(here, z_send.at[sem_in], z_recv.at[sem_in], sender[direction])
                o_ref[span] = o_ref[span] + here[...].astype(jnp.float32)

    key = (mid + 1) * count
    wait_arrival(a_got, y_send.at[key], y_recv.at[key], other)
    o_ref[first] = o_ref[first] + a_got[...].astype(jnp.float32)
    copies.finish()


def scatter_rows(partial, parts=1):
    n, rows, columns = partial.shape
    if not use_kernels(n, rows):
        return lax.psum_scatter(
            partial.reshape(n * rows, columns), "shard", scatter_dimension=0, tiled=True
        ).astype(jnp.float32)
    across, chunks = split_rows(rows)
    length, count = n // 2, len(chunks)
    late = rows - across
    keys = (2 * length - 1) * count + 1
    dtype = partial.dtype
    return pl.pallas_call(
        functools.partial(scatter_kernel, n, across, chunks),
        out_shape=jax.ShapeDtypeStruct((rows, columns), jnp.float32),
        in_specs=[pl.BlockSpec(memory_space=pltpu.VMEM)],
        out_specs=pl.BlockSpec(memory_space=pltpu.VMEM),
        scratch_shapes=[
            pltpu.VMEM((2 * length - 1, late, columns), dtype),
            pltpu.VMEM((2, length - 1, across + rows, columns), dtype),
            pltpu.VMEM((across, columns), dtype),
            pltpu.VMEM((across, columns), dtype),
            pltpu.SemaphoreType.DMA((2, length - 1, count + 2)),
            pltpu.SemaphoreType.DMA((2, length - 1, count + 2)),
            pltpu.SemaphoreType.DMA((keys,)),
            pltpu.SemaphoreType.DMA((keys,)),
        ],
        compiler_params=pltpu.CompilerParams(collective_id=10 + parts, has_side_effects=True),
        cost_estimate=wire_cost(n * rows * columns * 2),
        name="scatter_rows",
    )(partial)


def small_gather_kernel(n, a_ref, b_ref, a_out, b_out, send, recv):
    me = lax.axis_index("shard")
    barrier = pltpu.get_barrier_semaphore()
    peers = [lax.rem(me + d, n) for d in range(1, n)]
    for peer in peers:
        pl.semaphore_signal(barrier, inc=1, device_id={"shard": peer}, device_id_type=MESH)
    pl.semaphore_wait(barrier, n - 1)
    copies = Copies()
    for d, peer in enumerate(peers):
        for k, (src, dst) in enumerate(((a_ref, a_out), (b_ref, b_out))):
            copies.start(None, src, dst.at[me], send.at[k, d], recv.at[k, d], peer)
    a_out[me] = a_ref[...]
    b_out[me] = b_ref[...]
    for d in range(1, n):
        source = lax.rem(me + n - d, n)
        for k, dst in enumerate((a_out, b_out)):
            wait_arrival(dst.at[source], send.at[k, d - 1], recv.at[k, d - 1], source)
    copies.finish()


def gather_small(gains, segment_ids):
    n = lax.axis_size("shard")
    width, length = gains.shape[1], segment_ids.shape[1]
    if not use_kernels(n, 256) or width % 128 or length % 128:
        gains = lax.all_gather(gains, "shard", axis=1, tiled=True)
        return gains, lax.all_gather(segment_ids, "shard", axis=0, tiled=True)
    gains = jnp.pad(gains.astype(jnp.float32), ((0, 6), (0, 0)))
    ids = jnp.broadcast_to(segment_ids, (8, length))
    all_gains, all_ids = pl.pallas_call(
        functools.partial(small_gather_kernel, n),
        out_shape=(
            jax.ShapeDtypeStruct((n, 8, width), jnp.float32),
            jax.ShapeDtypeStruct((n, 8, length), jnp.int32),
        ),
        in_specs=[pl.BlockSpec(memory_space=pltpu.VMEM)] * 2,
        out_specs=[pl.BlockSpec(memory_space=pltpu.VMEM)] * 2,
        scratch_shapes=[pltpu.SemaphoreType.DMA((2, n - 1)), pltpu.SemaphoreType.DMA((2, n - 1))],
        compiler_params=pltpu.CompilerParams(collective_id=3, has_side_effects=True),
        name="gather_small",
    )(gains, ids)
    return all_gains[:, :2].transpose(1, 0, 2).reshape(2, n * width), all_ids[:, 0]


def small_sum_kernel(n, m, t_ref, o_ref, got, mine, shared, send, recv, send_two, recv_two):
    me, copy = lax.axis_index("shard"), lax.axis_index("replica")
    barrier = pltpu.get_barrier_semaphore()
    peers = [lax.rem(me + d, n) for d in range(1, n)]
    twins = [lax.rem(copy + d, m) for d in range(1, m)]
    for peer in peers:
        pl.semaphore_signal(barrier, inc=1, device_id={"shard": peer}, device_id_type=MESH)
    for twin in twins:
        pl.semaphore_signal(barrier, inc=1, device_id={"replica": twin}, device_id_type=MESH)
    pl.semaphore_wait(barrier, n + m - 2)
    copies = Copies()
    for d, peer in enumerate(peers):
        copies.start(None, t_ref.at[peer], got.at[me], send.at[d], recv.at[d], peer)
    got[me] = t_ref[me]
    for d in range(1, n):
        source = lax.rem(me + n - d, n)
        wait_arrival(got.at[source], send.at[d - 1], recv.at[d - 1], source)
    total = got[0]
    for i in range(1, n):
        total = total + got[i]
    mine[...] = total
    shared[copy] = total
    for d, twin in enumerate(twins):
        copies.start(
            None, mine, shared.at[copy], send_two.at[d], recv_two.at[d], twin, axis="replica"
        )
    for d in range(1, m):
        source = lax.rem(copy + m - d, m)
        wait_arrival(
            shared.at[source], send_two.at[d - 1], recv_two.at[d - 1], source, axis="replica"
        )
    total = shared[0]
    for i in range(1, m):
        total = total + shared[i]
    o_ref[...] = total
    copies.finish()


def sum_small(terms):
    n, m = lax.axis_size("shard"), lax.axis_size("replica")
    width = terms.shape[1] // n
    if not use_kernels(n, 256) or width % 128:
        total = lax.psum(terms, ("replica", "shard"))
        return lax.dynamic_slice_in_dim(total, lax.axis_index("shard") * width, width, axis=1)
    pieces = jnp.pad(terms, ((0, 6), (0, 0))).reshape(8, n, width).transpose(1, 0, 2)
    return pl.pallas_call(
        functools.partial(small_sum_kernel, n, m),
        out_shape=jax.ShapeDtypeStruct((8, width), jnp.float32),
        in_specs=[pl.BlockSpec(memory_space=pltpu.VMEM)],
        out_specs=pl.BlockSpec(memory_space=pltpu.VMEM),
        scratch_shapes=[
            pltpu.VMEM((n, 8, width), jnp.float32),
            pltpu.VMEM((8, width), jnp.float32),
            pltpu.VMEM((m, 8, width), jnp.float32),
            pltpu.SemaphoreType.DMA((n - 1,)),
            pltpu.SemaphoreType.DMA((n - 1,)),
            pltpu.SemaphoreType.DMA((m - 1,)),
            pltpu.SemaphoreType.DMA((m - 1,)),
        ],
        compiler_params=pltpu.CompilerParams(collective_id=4, has_side_effects=True),
        name="sum_small",
    )(pieces)[:2]


def after(x, *others):
    return lax.optimization_barrier((x,) + others)[0]


def swap_blocks(blocks, hold):
    n = blocks.shape[0]
    turned = jnp.roll(blocks, -lax.axis_index("shard"), axis=0)
    came = [turned[0]]
    for d in range(1, n):
        ring = [(i, (i - d) % n) for i in range(n)]
        came.append(lax.ppermute(turned[n - d], "shard", ring))
    came = lax.optimization_barrier((hold, *came))[1:]
    return jnp.stack(came)


def quarters(weights):
    n, copies = lax.axis_size("shard"), lax.axis_size("replica")
    part = weights[0].shape[0] // copies
    me = lax.axis_index("replica")
    pieces = [
        lax.dynamic_slice_in_dim(w, me * part, part).reshape(part, n, -1).transpose(1, 0, 2)
        for w in weights
    ]
    return jnp.concatenate(pieces, axis=2)


def share_two(came):
    m = lax.axis_size("replica")
    return lax.ppermute(came, "replica", [(i, (i + 2) % m) for i in range(m)])


def share_one(two):
    m = lax.axis_size("replica")
    return lax.ppermute(two, "replica", [(i, i + 1 - 2 * (i % 2)) for i in range(m)])


def merge_kernel(widths, by_column, at_ref, *refs):
    pieces, outs = refs[:4], refs[4:]
    part = pieces[0].shape[1]
    rank = at_ref[1]
    high, low = rank // 2, rank % 2
    ranks = (rank, 2 * (1 - high) + low, 2 * high + 1 - low, 2 * (1 - high) + 1 - low)
    for piece, other in zip(pieces, ranks):
        rows = pl.ds(pl.multiple_of(other * part, part), part)
        at = 0
        for width, out in zip(widths, outs):
            out[rows] = piece[0, :, pl.ds(at, width)].astype(out.dtype)
            at += width


def merge(pieces, widths, by_column):
    n, part, total = pieces[0].shape
    rows = 4 * part
    at = jnp.stack([lax.axis_index("shard"), lax.axis_index("replica")]).astype(jnp.int32)
    came = [pl.BlockSpec((1, part, total), lambda i, at: (lax.rem(i + n - at[0], n), 0, 0))] * 4
    if by_column:
        out_shape = [jax.ShapeDtypeStruct((rows, n * width), jnp.float32) for width in widths]
        out_specs = [pl.BlockSpec((rows, width), lambda i, at: (0, i)) for width in widths]
    else:
        widths = (total,)
        out_shape = [jax.ShapeDtypeStruct((n * rows, total), pieces[0].dtype)]
        out_specs = [pl.BlockSpec((rows, total), lambda i, at: (i, 0))]
    return pl.pallas_call(
        functools.partial(merge_kernel, widths, by_column),
        grid_spec=pltpu.PrefetchScalarGridSpec(
            num_scalar_prefetch=1, grid=(n,), in_specs=came, out_specs=out_specs
        ),
        out_shape=out_shape,
        name="merge",
    )(at, *pieces)


def can_merge(n, part, width):
    return lax.axis_size("replica") == 4 and part % 16 == 0 and width % 128 == 0


def turned_back(came):
    return jnp.roll(came, lax.axis_index("shard"), axis=0)


def as_columns(came, two, one, widths):
    n, part, total = came.shape
    if can_merge(n, part, total):
        return merge((came, two, one[0], one[1]), widths, False)[0]
    shared = lax.all_gather(turned_back(came), "replica", axis=1, tiled=False)
    return shared.reshape(-1, total)


def as_rows(came, two, one, widths):
    n, part, total = came.shape
    if all(can_merge(n, part, width) for width in widths):
        return merge((came, two, one[0], one[1]), widths, True)
    shared = lax.all_gather(turned_back(came), "replica", axis=0, tiled=False)
    out, at = [], 0
    for width in widths:
        piece = shared[..., at : at + width].transpose(0, 2, 1, 3).reshape(-1, n * width)
        out.append(piece.astype(jnp.float32))
        at += width
    return out


def sum_copies(grads):
    n, copies = lax.axis_size("shard"), lax.axis_size("replica")
    rows, width = grads.shape[0] // n, grads.shape[1]
    split = grads.reshape(n, copies, rows // copies, width).transpose(1, 0, 2, 3)
    return lax.psum_scatter(split, "replica", scatter_dimension=0, tiled=False)


def positions_tables(segment_rows, head_dim):
    length_all = segment_rows.shape[1]
    counter = lax.broadcasted_iota(jnp.int32, segment_rows.shape, 1)
    is_first = jnp.concatenate(
        [
            jnp.ones((segment_rows.shape[0], 1), jnp.bool_),
            segment_rows[:, 1:] != segment_rows[:, :-1],
        ],
        axis=1,
    )
    first_at = lax.cummax(jnp.where(is_first, counter, jnp.zeros_like(counter)), axis=1)
    position = (counter - first_at).astype(jnp.float32).reshape(-1)
    half_dim = head_dim // 2
    inverse = jnp.exp(
        -(jnp.arange(half_dim, dtype=jnp.float32) * (2.0 / head_dim)) * math.log(THETA)
    )
    angles = position[:, None] * inverse[None, :]
    return (jnp.cos(angles), jnp.sin(angles))


def rotate(values, cosine, sine_tab, direction, head_dim):
    row_count, total_width = values.shape
    half_dim = head_dim // 2
    halves = values.reshape(row_count, total_width // head_dim, 2, half_dim)
    first_half = halves[:, :, 0]
    second_half = halves[:, :, 1]
    cos_wide = cosine[:, None, :]
    sin_wide = direction * sine_tab[:, None, :]
    turned = jnp.stack(
        [
            first_half * cos_wide - second_half * sin_wide,
            second_half * cos_wide + first_half * sin_wide,
        ],
        axis=2,
    )
    return turned.reshape(row_count, total_width)


def allowed(segment_rows):
    ids = jnp.arange(segment_rows.shape[1], dtype=jnp.int32)
    return (segment_rows[:, :, None] == segment_rows[:, None, :]) & (
        ids[None, None, :] <= ids[None, :, None]
    )


def heads_of(values, packs, head_dim):
    return values.reshape(packs, values.shape[0] // packs, -1, head_dim)


def pair_scores(q_heads, k_heads, mask):
    scores = (
        jnp.einsum("pqhd,pkhd->phqk", q_heads, k_heads, preferred_element_type=jnp.float32) * SCALE
    )
    return jnp.where(mask[:, None], scores, -1e30)


def attention_forward(q_rot, k_rot, v_vals, segment_rows, head_dim):
    packs = segment_rows.shape[0]
    q_heads, k_heads, v_heads = (heads_of(v, packs, head_dim) for v in (q_rot, k_rot, v_vals))
    scores = pair_scores(q_heads, k_heads, allowed(segment_rows))
    log_total = jnp.log(jnp.sum(jnp.exp(scores), axis=-1))
    rounded_probs = jnp.exp(scores - log_total[..., None]).astype(jnp.bfloat16)
    mixed_out = jnp.einsum(
        "phqk,pkhd->pqhd", rounded_probs, v_heads, preferred_element_type=jnp.float32
    )
    return mixed_out.astype(jnp.bfloat16).reshape(q_rot.shape), log_total


def attention_backward(q_rot, k_rot, v_vals, log_total, grad_att, segment_rows, head_dim):
    packs = segment_rows.shape[0]
    q_heads, k_heads, v_heads, g_heads = (
        heads_of(v, packs, head_dim) for v in (q_rot, k_rot, v_vals, grad_att)
    )
    scores = pair_scores(q_heads, k_heads, allowed(segment_rows))
    attn_probs = jnp.exp(scores - log_total[..., None])
    grad_probs = jnp.einsum("pqhd,pkhd->phqk", g_heads, v_heads, preferred_element_type=jnp.float32)
    inner_sum = jnp.sum(attn_probs * grad_probs, axis=-1, keepdims=True)
    grad_scores = (attn_probs * (grad_probs - inner_sum) * SCALE).astype(jnp.bfloat16)
    rounded_probs = attn_probs.astype(jnp.bfloat16)
    grad_q = jnp.einsum("phqk,pkhd->pqhd", grad_scores, k_heads, preferred_element_type=jnp.float32)
    grad_k = jnp.einsum("phqk,pqhd->pkhd", grad_scores, q_heads, preferred_element_type=jnp.float32)
    grad_v = jnp.einsum(
        "phqk,pqhd->pkhd", rounded_probs, g_heads, preferred_element_type=jnp.float32
    )
    return tuple(g.reshape(q_rot.shape) for g in (grad_q, grad_k, grad_v))


def turn(values, cosine, sine_tab, direction):
    lane = lax.broadcasted_iota(jnp.int32, values.shape, 1)
    is_first = lane % HEAD_DIM < HEAD_DIM // 2
    width = values.shape[1]
    swapped = jnp.where(
        is_first,
        pltpu.roll(values, width - HEAD_DIM // 2, 1),
        pltpu.roll(values, HEAD_DIM // 2, 1),
    )
    return values * cosine + swapped * jnp.where(is_first, -direction, direction) * sine_tab


def head_probs(q_head, k_head, mask):
    scores = jnp.where(mask, times_transposed(q_head, k_head) * SCALE, -1e30)
    log_total = jnp.log(jnp.sum(jnp.exp(scores), axis=-1, keepdims=True))
    return jnp.exp(scores - log_total)


def attend_kernel(width, qkv_ref, cos_ref, sin_ref, mask_ref, rot_ref, att_ref):
    cosine, sine_tab = cos_ref[...], sin_ref[...]
    mask = mask_ref[0] > 0.5
    lanes = 2 * HEAD_DIM
    for at in range(0, width, lanes):
        q_two = turn(qkv_ref[:, at : at + lanes], cosine, sine_tab, 1.0).astype(jnp.bfloat16)
        k_at, v_at = width + at, 2 * width + at
        k_two = turn(qkv_ref[:, k_at : k_at + lanes], cosine, sine_tab, 1.0).astype(jnp.bfloat16)
        v_two = qkv_ref[:, v_at : v_at + lanes].astype(jnp.bfloat16)
        rot_ref[:, at : at + lanes] = q_two
        rot_ref[:, k_at : k_at + lanes] = k_two
        rot_ref[:, v_at : v_at + lanes] = v_two
        mixed = []
        for h in range(0, lanes, HEAD_DIM):
            one = slice(h, h + HEAD_DIM)
            probs = head_probs(q_two[:, one], k_two[:, one], mask).astype(jnp.bfloat16)
            mixed.append(times_plain(probs, v_two[:, one]))
        att_ref[:, at : at + lanes] = jnp.concatenate(mixed, axis=1).astype(att_ref.dtype)


def attend_back_kernel(width, rot_ref, g_ref, cos_ref, sin_ref, mask_ref, back_ref):
    cosine, sine_tab = cos_ref[...], sin_ref[...]
    mask = mask_ref[0] > 0.5
    lanes = 2 * HEAD_DIM
    for at in range(0, width, lanes):
        k_at, v_at = width + at, 2 * width + at
        q_two = rot_ref[:, at : at + lanes]
        k_two = rot_ref[:, k_at : k_at + lanes]
        v_two = rot_ref[:, v_at : v_at + lanes]
        g_two = g_ref[:, at : at + lanes]
        grads = ([], [], [])
        for h in range(0, lanes, HEAD_DIM):
            one = slice(h, h + HEAD_DIM)
            q, k, v, g = q_two[:, one], k_two[:, one], v_two[:, one], g_two[:, one]
            probs = head_probs(q, k, mask)
            grad_probs = times_transposed(g, v)
            inner = jnp.sum(probs * grad_probs, axis=-1, keepdims=True)
            grad_scores = (probs * (grad_probs - inner) * SCALE).astype(jnp.bfloat16)
            grads[0].append(times_plain(grad_scores, k))
            grads[1].append(token_contract(grad_scores, q))
            grads[2].append(token_contract(probs.astype(jnp.bfloat16), g))
        grad_q, grad_k, grad_v = (jnp.concatenate(g, axis=1) for g in grads)
        dtype = back_ref.dtype
        back_ref[:, at : at + lanes] = turn(grad_q, cosine, sine_tab, -1.0).astype(dtype)
        back_ref[:, k_at : k_at + lanes] = turn(grad_k, cosine, sine_tab, -1.0).astype(dtype)
        back_ref[:, v_at : v_at + lanes] = grad_v.astype(dtype)


def pack_specs(length, *widths):
    return [pl.BlockSpec((length, width), lambda i: (i, 0)) for width in widths]


def wide_tables(segment_rows):
    cosine, sine_tab = positions_tables(segment_rows, HEAD_DIM)
    mask = allowed(segment_rows).astype(jnp.float32)
    return jnp.tile(cosine, (1, 4)), jnp.tile(sine_tab, (1, 4)), mask


def attend(qkv, tables):
    cosine, sine_tab, mask = tables
    packs, length, _ = mask.shape
    tokens, width = qkv.shape[0], qkv.shape[1] // 3
    return pl.pallas_call(
        functools.partial(attend_kernel, width),
        grid=(packs,),
        out_shape=[
            jax.ShapeDtypeStruct((tokens, 3 * width), jnp.bfloat16),
            jax.ShapeDtypeStruct((tokens, width), jnp.bfloat16),
        ],
        in_specs=pack_specs(length, 3 * width, 2 * HEAD_DIM, 2 * HEAD_DIM)
        + [pl.BlockSpec((1, length, length), lambda i: (i, 0, 0))],
        out_specs=pack_specs(length, 3 * width, width),
        name="attend",
    )(qkv, cosine, sine_tab, mask)


def attend_back(rotated, grad_att, tables):
    cosine, sine_tab, mask = tables
    packs, length, _ = mask.shape
    tokens, width = grad_att.shape
    return pl.pallas_call(
        functools.partial(attend_back_kernel, width),
        grid=(packs,),
        out_shape=jax.ShapeDtypeStruct((tokens, 3 * width), jnp.bfloat16),
        in_specs=pack_specs(length, 3 * width, width, 2 * HEAD_DIM, 2 * HEAD_DIM)
        + [pl.BlockSpec((1, length, length), lambda i: (i, 0, 0))],
        out_specs=pack_specs(length, 3 * width)[0],
        name="attend_back",
    )(rotated, grad_att, cosine, sine_tab, mask)


def attend_plain(qkv, segment_rows):
    width = qkv.shape[1] // 3
    cosine, sine_tab = positions_tables(segment_rows, HEAD_DIM)
    q_rot = rotate(qkv[:, :width], cosine, sine_tab, 1.0, HEAD_DIM).astype(jnp.bfloat16)
    k_rot = rotate(qkv[:, width : 2 * width], cosine, sine_tab, 1.0, HEAD_DIM).astype(jnp.bfloat16)
    v_vals = qkv[:, 2 * width :].astype(jnp.bfloat16)
    attended, log_total = attention_forward(q_rot, k_rot, v_vals, segment_rows, HEAD_DIM)
    return (q_rot, k_rot, v_vals, log_total), attended


def attend_back_plain(rotated, grad_att, segment_rows):
    cosine, sine_tab = positions_tables(segment_rows, HEAD_DIM)
    q_rot, k_rot, v_vals, log_total = rotated
    grad_q, grad_k, grad_v = attention_backward(
        q_rot, k_rot, v_vals, log_total, grad_att, segment_rows, HEAD_DIM
    )
    q_back = rotate(grad_q, cosine, sine_tab, -1.0, HEAD_DIM)
    k_back = rotate(grad_k, cosine, sine_tab, -1.0, HEAD_DIM)
    return jnp.concatenate([q_back, k_back, grad_v], axis=1).astype(jnp.bfloat16)


def norm_scale(values):
    return lax.rsqrt(jnp.mean(values * values, axis=-1, keepdims=True) + EPS)


def norm_back(upstream, source, scale, gain, grad_normed):
    gain_term = jnp.sum(grad_normed * source * scale, axis=0)
    weighted = gain * grad_normed
    grad = (
        upstream
        + scale * weighted
        - source * (scale * scale * scale) * jnp.mean(weighted * source, axis=-1, keepdims=True)
    )
    return grad, gain_term


def per_device(
    block_input,
    segment_ids,
    attn_gain,
    mlp_gain,
    w_query,
    w_key,
    w_value,
    w_out,
    w_gate,
    w_up,
    w_down,
    out_grad,
):
    n = lax.axis_size("shard")
    row_count, model_width = block_input.shape

    def spread(x, parts=1):
        return gather_rows(x, parts).reshape(n * row_count, -1)

    def collect(partial):
        return scatter_rows(partial.astype(jnp.bfloat16).reshape(n, row_count, model_width))

    half, quarter = model_width // 2, model_width // 4
    qkv_quarter = quarters((w_query, w_key, w_value))
    pair_quarter = quarters((w_gate, w_up))
    head_width, ff_width = qkv_quarter.shape[2] // 3, pair_quarter.shape[2] // 2
    by_kernel = head_width % (2 * HEAD_DIM) == 0
    gains, segment_rows = gather_small(jnp.stack([attn_gain, mlp_gain]), segment_ids)
    gain_one, gain_two = gains[0].astype(jnp.float32), gains[1].astype(jnp.float32)

    input_f = block_input.astype(jnp.float32)
    scale_one = norm_scale(input_f)
    normed_own = (input_f * scale_one * gain_one).astype(jnp.bfloat16)
    first_one = spread(normed_own[:, :half], 2)
    qkv_came = swap_blocks(qkv_quarter, first_one)
    qkv_two = share_two(qkv_came)
    pair_came = swap_blocks(pair_quarter, first_one)
    second_one = spread(after(normed_own[:, half:], first_one, pair_came), 2)
    qkv_came, qkv_two, second_one = lax.optimization_barrier((qkv_came, qkv_two, second_one))
    qkv_one = share_one(jnp.stack([qkv_came, qkv_two]))
    pair_two = share_two(pair_came)
    cotangent = lax.all_gather(after(out_grad, second_one), "shard", axis=0, tiled=True)
    qkv_cols = as_columns(qkv_came, qkv_two, qkv_one, (head_width,) * 3)
    qkv = times_plain(first_one, qkv_cols[:half]) + times_plain(second_one, qkv_cols[half:])
    if by_kernel:
        tables = wide_tables(segment_rows)
        rotated, attended = attend(qkv, tables)
    else:
        rotated, attended = attend_plain(qkv, segment_rows)
    pair_came, pair_two, attended = lax.optimization_barrier((pair_came, pair_two, attended))
    pair_one = share_one(jnp.stack([pair_came, pair_two]))
    attn_rows = collect(times_plain(attended, w_out))
    pair_cols = as_columns(pair_came, pair_two, after(pair_one, attn_rows), (ff_width,) * 2)
    residual = input_f + attn_rows
    scale_two = norm_scale(residual)
    normed_two = spread((residual * scale_two * gain_two).astype(jnp.bfloat16))
    pair_pre = times_plain(normed_two, pair_cols)
    gate_pre, up_pre = pair_pre[:, :ff_width], pair_pre[:, ff_width:]
    gate_sig = jax.nn.sigmoid(gate_pre)
    silu_val = gate_pre * gate_sig
    hidden_b = (silu_val * up_pre).astype(jnp.bfloat16)

    grad_hidden = times_transposed(cotangent, w_down)
    gate_b = (grad_hidden * up_pre * gate_sig * (1.0 + gate_pre * (1.0 - gate_sig))).astype(
        jnp.bfloat16
    )
    up_b = (grad_hidden * silu_val).astype(jnp.bfloat16)
    pair_b = jnp.concatenate([gate_b, up_b], axis=1)
    pair_sum = sum_copies(token_contract(normed_two, pair_b).astype(jnp.bfloat16))
    mlp_partial, pair_b = lax.optimization_barrier(
        (times_plain(hidden_b, w_down).astype(jnp.bfloat16), pair_b)
    )
    mlp_rows = lax.psum_scatter(
        mlp_partial,
        "shard",
        scatter_dimension=0,
        tiled=True,
    )
    grad_normed_two = collect(times_transposed(pair_b, pair_cols))
    pair_sum, grad_normed_two = lax.optimization_barrier((pair_sum, grad_normed_two))
    grad_residual, gain_two_term = norm_back(
        out_grad.astype(jnp.float32), residual, scale_two, gain_two, grad_normed_two
    )
    residual_b = spread(grad_residual.astype(jnp.bfloat16))
    pair_came = swap_blocks(pair_sum, residual_b)
    pair_two = share_two(pair_came)
    grad_att = times_transposed(residual_b, w_out).astype(jnp.bfloat16)
    if by_kernel:
        back = attend_back(rotated, grad_att, tables)
    else:
        back = attend_back_plain(rotated, grad_att, segment_rows)
    pair_came, pair_two, back = lax.optimization_barrier((pair_came, pair_two, back))
    pair_one = share_one(jnp.stack([pair_came, pair_two]))
    qkv_sum = sum_copies(
        jnp.concatenate([token_contract(first_one, back), token_contract(second_one, back)]).astype(
            jnp.bfloat16
        )
    )
    grad_out = token_contract(attended, residual_b).astype(jnp.bfloat16)
    grad_down = token_contract(hidden_b, cotangent).astype(jnp.bfloat16)
    mlp_rows, back = lax.optimization_barrier((mlp_rows, back))
    partial_one = times_transposed(back, qkv_cols).astype(jnp.bfloat16)
    partial_one = partial_one.reshape(n, row_count, model_width)
    piece_a = scatter_rows(partial_one[:, :, :half], 2)
    qkv_sum, piece_a = lax.optimization_barrier((qkv_sum, piece_a))
    piece_b = scatter_rows(after(partial_one[:, :, half : half + quarter], piece_a), 4)
    qkv_came = swap_blocks(qkv_sum, piece_b)
    qkv_two = share_two(qkv_came)
    grad_out, grad_down = (
        lax.psum(g, "replica") for g in lax.optimization_barrier((grad_out, grad_down, qkv_sum))[:2]
    )
    piece_c = scatter_rows(after(partial_one[:, :, half + quarter :], piece_b), 4)
    qkv_came, qkv_two, piece_c = lax.optimization_barrier((qkv_came, qkv_two, piece_c))
    qkv_one = share_one(jnp.stack([qkv_came, qkv_two]))
    grad_normed_one = jnp.concatenate([piece_a, piece_b, piece_c], axis=1)
    input_grad, gain_one_term = norm_back(
        grad_residual, input_f, scale_one, gain_one, grad_normed_one
    )
    gain_rows = sum_small(jnp.stack([gain_one_term, gain_two_term]))
    grad_gate, grad_up = as_rows(
        pair_came, pair_two, after(pair_one, piece_c), (ff_width, ff_width)
    )
    block_output = (residual + after(mlp_rows, piece_c).astype(jnp.float32)).astype(jnp.bfloat16)
    grad_query, grad_key, grad_value = as_rows(qkv_came, qkv_two, qkv_one, (head_width,) * 3)
    return (
        block_output,
        input_grad,
        grad_query,
        grad_key,
        grad_value,
        grad_out.astype(jnp.float32),
        grad_gate,
        grad_up,
        grad_down.astype(jnp.float32),
        gain_rows[0],
        gain_rows[1],
    )


def solution(mesh):
    placed = (
        P(("replica", "shard"), None),
        P(("replica", "shard"), None),
        P("shard"),
        P("shard"),
        P("shard", None),
        P("shard", None),
        P("shard", None),
        P("shard", None),
        P("shard", None),
        P("shard", None),
        P("shard", None),
        P(("replica", "shard"), None),
    )
    return jax.shard_map(
        per_device,
        mesh=mesh,
        in_specs=placed,
        out_specs=(
            P(("replica", "shard"), None),
            P(("replica", "shard"), None),
            P("shard", None),
            P("shard", None),
            P("shard", None),
            P("shard", None),
            P("shard", None),
            P("shard", None),
            P("shard", None),
            P("shard"),
            P("shard"),
        ),
        check_vma=False,
    )
```

```python
import functools
import math

import jax
import jax.numpy as jnp
from jax import lax
from jax.experimental import pallas as pl
from jax.experimental.pallas import tpu as pltpu
from jax.sharding import PartitionSpec as P

MESH = pl.DeviceIdType.MESH

HEAD_DIM = 64


EPS = 1e-05
THETA = 130000.0
SCALE = 0.125


def times_plain(left_op, right_op):
    return jnp.dot(left_op, right_op, preferred_element_type=jnp.float32)


def times_transposed(left_op, right_op):
    return lax.dot_general(
        left_op, right_op, (((1,), (1,)), ((), ())), preferred_element_type=jnp.float32
    )


def token_contract(left_op, right_op):
    return lax.dot_general(
        left_op, right_op, (((0,), (0,)), ((), ())), preferred_element_type=jnp.float32
    )


def split_rows(rows):
    unit = 16
    across = (rows // unit) * 3 // 16 * unit
    rest = (rows - across) // unit
    count = min(4, rest)
    sizes = [(rest // count + (1 if i >= count - rest % count else 0)) * unit for i in range(count)]
    chunks, at = [], across
    for size in sizes:
        chunks.append((at, size))
        at += size
    return across, chunks


def use_kernels(n, rows):
    return n % 2 == 0 and 2 < n <= 8 and rows % 256 == 0


def wire_cost(size):
    return pl.CostEstimate(flops=0, bytes_accessed=30 * size, transcendentals=0)


class Copies:
    def __init__(self):
        self.started = []

    def start(self, cond, src, dst, send_sem, recv_sem, target, axis="shard"):
        copy = pltpu.make_async_remote_copy(
            src_ref=src,
            dst_ref=dst,
            send_sem=send_sem,
            recv_sem=recv_sem,
            device_id={axis: target},
            device_id_type=MESH,
        )
        if cond is None:
            copy.start()
        else:
            pl.when(cond)(copy.start)
        self.started.append((cond, copy))

    def finish(self):
        for cond, copy in self.started:
            if cond is None:
                copy.wait_send()
            else:
                pl.when(cond)(copy.wait_send)


def wait_arrival(dst, send_sem, recv_sem, source, axis="shard"):
    pltpu.make_async_remote_copy(
        src_ref=dst,
        dst_ref=dst,
        send_sem=send_sem,
        recv_sem=recv_sem,
        device_id={axis: source},
        device_id_type=MESH,
    ).wait_recv()


def greet_all(n, me):
    barrier = pltpu.get_barrier_semaphore()
    for d in range(1, n):
        pl.semaphore_signal(
            barrier, inc=1, device_id={"shard": lax.rem(me + d, n)}, device_id_type=MESH
        )
    pl.semaphore_wait(barrier, n - 1)


class Swaps:
    def __init__(self, n, me, sources, targets, send, recv):
        self.n, self.me, self.send, self.recv = n, me, send, recv
        self.pairs = list(zip(sources, targets))

    def start(self, copies):
        for d in range(1, self.n):
            peer = lax.rem(self.me + d, self.n)
            for k, (source, target) in enumerate(self.pairs):
                copies.start(
                    None,
                    source.at[peer],
                    target.at[self.me],
                    self.send.at[k, d - 1],
                    self.recv.at[k, d - 1],
                    peer,
                )
        for source, target in self.pairs:
            target[self.me] = source[self.me]

    def wait(self):
        for d in range(1, self.n):
            sender = lax.rem(self.me + self.n - d, self.n)
            for k, (_, target) in enumerate(self.pairs):
                wait_arrival(
                    target.at[sender], self.send.at[k, d - 1], self.recv.at[k, d - 1], sender
                )


def swap_scratch(n, swaps):
    return [pltpu.SemaphoreType.DMA((max(len(swaps), 1), n - 1))] * 2


def swap_plain(swaps):
    return [lax.all_to_all(s, "shard", split_axis=0, concat_axis=0, tiled=True) for s in swaps]


def greet(has_left, has_right, left, right, other):
    barrier = pltpu.get_barrier_semaphore()
    pl.semaphore_signal(barrier, inc=1, device_id={"shard": other}, device_id_type=MESH)

    @pl.when(has_left)
    def _():
        pl.semaphore_signal(barrier, inc=1, device_id={"shard": left}, device_id_type=MESH)

    @pl.when(has_right)
    def _():
        pl.semaphore_signal(barrier, inc=1, device_id={"shard": right}, device_id_type=MESH)

    pl.semaphore_wait(barrier, 1 + has_left.astype(jnp.int32) + has_right.astype(jnp.int32))


def gather_kernel(n, across, chunks, n_swaps, *refs):
    x_ref, swap_in = refs[0], refs[1 : 1 + n_swaps]
    o_ref, swap_out = refs[1 + n_swaps], refs[2 + n_swaps : 2 + 2 * n_swaps]
    own_sem, z_send, z_recv, y_send, y_recv, s_send, s_recv = refs[2 + 2 * n_swaps :]
    length = n // 2
    count = len(chunks)
    me = lax.axis_index("shard")
    place, side = me // 2, me % 2
    other = me + 1 - 2 * side
    has_left, has_right = place > 0, place < length - 1
    nexts = ((has_right, me + 2), (has_left, me - 2))
    if n_swaps:
        greet_all(n, me)
    else:
        greet(has_left, has_right, me - 2, me + 2, other)
    swaps = Swaps(n, me, swap_in, swap_out, s_send, s_recv)
    copies = Copies()
    own = pltpu.make_async_copy(x_ref, o_ref.at[me], own_sem)
    own.start()
    first = pl.ds(0, across)
    y_first = (2 * length - 1) * count
    copies.start(
        None, x_ref.at[first], o_ref.at[me, first], y_send.at[y_first], y_recv.at[y_first], other
    )

    def z_hop(direction, hop, slot, src, dst):
        cond, target = nexts[direction]
        copies.start(
            cond,
            src,
            dst,
            z_send.at[direction, hop, slot],
            z_recv.at[direction, hop, slot],
            target,
        )

    def y_hop(origin, chunk, src, dst, cond, key):
        copies.start(cond, src, dst, y_send.at[key], y_recv.at[key], other)

    for c, (at, size) in enumerate(chunks):
        span = pl.ds(at, size)
        for direction in range(2):
            z_hop(direction, 0, c, x_ref.at[span], o_ref.at[me, span])
        y_hop(me, c, x_ref.at[span], o_ref.at[me, span], None, c)
    swaps.start(copies)
    for hop in range(1, length):
        for c, (at, size) in enumerate(chunks):
            span = pl.ds(at, size)
            for direction in range(2):
                source = me - 2 * hop if direction == 0 else me + 2 * hop
                exists = source >= 0 if direction == 0 else source < n
                sender = me - 2 if direction == 0 else me + 2

                @pl.when(exists)
                def _():
                    wait_arrival(
                        o_ref.at[source, span],
                        z_send.at[direction, hop - 1, c],
                        z_recv.at[direction, hop - 1, c],
                        sender,
                    )

                here = o_ref.at[source, span]
                if hop < length - 1:
                    cond, target = nexts[direction]
                    copies.start(
                        jnp.logical_and(exists, cond),
                        here,
                        here,
                        z_send.at[direction, hop, c],
                        z_recv.at[direction, hop, c],
                        target,
                    )
                key = (1 + direction * (length - 1) + hop - 1) * count + c
                copies.start(exists, here, here, y_send.at[key], y_recv.at[key], other)
    wait_arrival(o_ref.at[other, first], y_send.at[y_first], y_recv.at[y_first], other)
    for direction in range(2):
        z_hop(direction, 0, count, x_ref.at[first], o_ref.at[me, first])
        z_hop(direction, 0, count + 1, o_ref.at[other, first], o_ref.at[other, first])
    for hop in range(1, length):
        for line, base in enumerate((me, other)):
            for direction in range(2):
                source = base - 2 * hop if direction == 0 else base + 2 * hop
                exists = source >= 0 if direction == 0 else source < n
                sender = me - 2 if direction == 0 else me + 2

                @pl.when(exists)
                def _():
                    wait_arrival(
                        o_ref.at[source, first],
                        z_send.at[direction, hop - 1, count + line],
                        z_recv.at[direction, hop - 1, count + line],
                        sender,
                    )

                here = o_ref.at[source, first]
                if hop < length - 1:
                    cond, target = nexts[direction]
                    copies.start(
                        jnp.logical_and(exists, cond),
                        here,
                        here,
                        z_send.at[direction, hop, count + line],
                        z_recv.at[direction, hop, count + line],
                        target,
                    )
    for c, (at, size) in enumerate(chunks):
        span = pl.ds(at, size)
        wait_arrival(o_ref.at[other, span], y_send.at[c], y_recv.at[c], other)
        for hop in range(1, length):
            for direction in range(2):
                source = other - 2 * hop if direction == 0 else other + 2 * hop
                exists = source >= 0 if direction == 0 else source < n
                key = (1 + direction * (length - 1) + hop - 1) * count + c

                @pl.when(exists)
                def _():
                    wait_arrival(o_ref.at[source, span], y_send.at[key], y_recv.at[key], other)

    own.wait()
    swaps.wait()
    copies.finish()


def gather_rows(x, ident, swaps=()):
    n = lax.axis_size("shard")
    rows, columns = x.shape
    if not use_kernels(n, rows):
        return lax.all_gather(x, "shard", axis=0, tiled=False), *swap_plain(swaps)
    across, chunks = split_rows(rows)
    length, count = n // 2, len(chunks)
    keys = (2 * length - 1) * count + 1
    return pl.pallas_call(
        functools.partial(gather_kernel, n, across, chunks, len(swaps)),
        out_shape=[jax.ShapeDtypeStruct((n, rows, columns), x.dtype)]
        + [jax.ShapeDtypeStruct(s.shape, s.dtype) for s in swaps],
        in_specs=[pl.BlockSpec(memory_space=pltpu.VMEM)] * (1 + len(swaps)),
        out_specs=[pl.BlockSpec(memory_space=pl.ANY)]
        + [pl.BlockSpec(memory_space=pltpu.VMEM)] * len(swaps),
        scratch_shapes=[
            pltpu.SemaphoreType.DMA,
            pltpu.SemaphoreType.DMA((2, length - 1, count + 2)),
            pltpu.SemaphoreType.DMA((2, length - 1, count + 2)),
            pltpu.SemaphoreType.DMA((keys,)),
            pltpu.SemaphoreType.DMA((keys,)),
        ]
        + swap_scratch(n, swaps),
        compiler_params=pltpu.CompilerParams(collective_id=5 + ident, has_side_effects=True),
        cost_estimate=wire_cost(n * rows * columns * 2),
        name="gather_rows",
    )(x, *swaps)


def add_rows(*terms):
    total = terms[0].astype(jnp.float32)
    for term in terms[1:]:
        total = total + term.astype(jnp.float32)
    return total


def scatter_kernel(n, across, chunks, n_swaps, *refs):
    p_ref, swap_in = refs[0], refs[1 : 1 + n_swaps]
    o_ref, swap_out = refs[1 + n_swaps], refs[2 + n_swaps : 2 + 2 * n_swaps]
    y_buf, z_buf, a_buf, a_got, z_send, z_recv, y_send, y_recv, s_send, s_recv = refs[
        2 + 2 * n_swaps :
    ]
    length = n // 2
    count = len(chunks)
    me = lax.axis_index("shard")
    place, side = me // 2, me % 2
    other = me + 1 - 2 * side
    has_left, has_right = place > 0, place < length - 1
    if n_swaps:
        greet_all(n, me)
    else:
        greet(has_left, has_right, me - 2, me + 2, other)
    swaps = Swaps(n, me, swap_in, swap_out, s_send, s_recv)
    copies = Copies()
    first = pl.ds(0, across)

    def routes():
        for distance in range(length - 1, 0, -1):
            yield 0, distance, place + distance, place + distance < length
            yield 1, distance, place - distance, place - distance >= 0

    behind = (has_left, has_right)
    sender = (me - 2, me + 2)
    target = (me + 2, me - 2)

    for direction, distance, owner, exists in routes():
        for c, (at, size) in enumerate(chunks):
            key = (direction * (length - 1) + distance - 1) * count + c
            copies.start(
                exists,
                p_ref.at[2 * owner + 1 - side, pl.ds(at, size)],
                y_buf.at[direction * (length - 1) + distance - 1, pl.ds(at - across, size)],
                y_send.at[key],
                y_recv.at[key],
                other,
            )
    mid = 2 * (length - 1)
    for c, (at, size) in enumerate(chunks):
        key = mid * count + c
        copies.start(
            None,
            p_ref.at[2 * place + 1 - side, pl.ds(at, size)],
            y_buf.at[mid, pl.ds(at - across, size)],
            y_send.at[key],
            y_recv.at[key],
            other,
        )

    swaps.start(copies)

    def z_dst(direction, distance, at, size):
        return z_buf.at[direction, distance, pl.ds(at, size)]

    for direction, distance, owner, exists in routes():
        for line in range(2):
            block = 2 * owner + (side if line == 0 else 1 - side)
            sem_in = (direction, distance, count + line)
            sem_out = (direction, distance - 1, count + line)
            place_rows = line * across
            from_start = jnp.logical_and(exists, jnp.logical_not(behind[direction]))
            passing = jnp.logical_and(exists, behind[direction])
            dst = z_dst(direction, distance - 1, place_rows, across)
            copies.start(
                from_start,
                p_ref.at[block, first],
                dst,
                z_send.at[sem_out],
                z_recv.at[sem_out],
                target[direction],
            )
            if distance < length - 1:
                here = z_dst(direction, distance, place_rows, across)

                @pl.when(passing)
                def _():
                    wait_arrival(here, z_send.at[sem_in], z_recv.at[sem_in], sender[direction])
                    here[...] = add_rows(here[...], p_ref[block, first]).astype(here.dtype)

                copies.start(
                    passing, here, dst, z_send.at[sem_out], z_recv.at[sem_out], target[direction]
                )

    for line in (1, 0):
        block = 2 * place + (side if line == 0 else 1 - side)
        o_ref[first] = p_ref[block, first].astype(jnp.float32)
        for direction in range(2):
            sem_in = (direction, 0, count + line)
            here = z_dst(direction, 0, line * across, across)

            @pl.when(behind[direction])
            def _():
                wait_arrival(here, z_send.at[sem_in], z_recv.at[sem_in], sender[direction])
                o_ref[first] = o_ref[first] + here[...].astype(jnp.float32)

        if line == 1:
            a_buf[...] = o_ref[first].astype(a_buf.dtype)
            key = (mid + 1) * count
            copies.start(None, a_buf, a_got, y_send.at[key], y_recv.at[key], other)

    for direction, distance, owner, exists in routes():
        slot = direction * (length - 1) + distance - 1
        for c, (at, size) in enumerate(chunks):
            key = slot * count + c
            held = y_buf.at[slot, pl.ds(at - across, size)]
            block = 2 * owner + side
            sem_in = (direction, distance, c)
            sem_out = (direction, distance - 1, c)
            rows_at = across + at
            span = pl.ds(at, size)

            @pl.when(exists)
            def _():
                wait_arrival(held, y_send.at[key], y_recv.at[key], other)

            if distance < length - 1:
                here = z_dst(direction, distance, rows_at, size)

                @pl.when(jnp.logical_and(exists, behind[direction]))
                def _():
                    wait_arrival(here, z_send.at[sem_in], z_recv.at[sem_in], sender[direction])
                    held[...] = add_rows(held[...], p_ref[block, span], here[...]).astype(
                        held.dtype
                    )

            @pl.when(jnp.logical_and(exists, jnp.logical_not(behind[direction])))
            def _():
                held[...] = add_rows(held[...], p_ref[block, span]).astype(held.dtype)

            copies.start(
                exists,
                held,
                z_dst(direction, distance - 1, rows_at, size),
                z_send.at[sem_out],
                z_recv.at[sem_out],
                target[direction],
            )
    for c, (at, size) in enumerate(chunks):
        key = mid * count + c
        held = y_buf.at[mid, pl.ds(at - across, size)]
        span = pl.ds(at, size)
        wait_arrival(held, y_send.at[key], y_recv.at[key], other)
        o_ref[span] = add_rows(held[...], p_ref[me, span])
        for direction in range(2):
            sem_in = (direction, 0, c)
            here = z_dst(direction, 0, across + at, size)

            @pl.when(behind[direction])
            def _():
                wait_arrival(here, z_send.at[sem_in], z_recv.at[sem_in], sender[direction])
                o_ref[span] = o_ref[span] + here[...].astype(jnp.float32)

    key = (mid + 1) * count
    wait_arrival(a_got, y_send.at[key], y_recv.at[key], other)
    o_ref[first] = o_ref[first] + a_got[...].astype(jnp.float32)
    swaps.wait()
    copies.finish()


def scatter_rows(partial, ident, swaps=()):
    n, rows, columns = partial.shape
    if not use_kernels(n, rows):
        total = lax.psum_scatter(
            partial.reshape(n * rows, columns), "shard", scatter_dimension=0, tiled=True
        )
        return total.astype(jnp.float32), *swap_plain(swaps)
    across, chunks = split_rows(rows)
    length, count = n // 2, len(chunks)
    late = rows - across
    keys = (2 * length - 1) * count + 1
    dtype = partial.dtype
    return pl.pallas_call(
        functools.partial(scatter_kernel, n, across, chunks, len(swaps)),
        out_shape=[jax.ShapeDtypeStruct((rows, columns), jnp.float32)]
        + [jax.ShapeDtypeStruct(s.shape, s.dtype) for s in swaps],
        in_specs=[pl.BlockSpec(memory_space=pltpu.VMEM)] * (1 + len(swaps)),
        out_specs=[pl.BlockSpec(memory_space=pltpu.VMEM)] * (1 + len(swaps)),
        scratch_shapes=[
            pltpu.VMEM((2 * length - 1, late, columns), dtype),
            pltpu.VMEM((2, length - 1, across + rows, columns), dtype),
            pltpu.VMEM((across, columns), dtype),
            pltpu.VMEM((across, columns), dtype),
            pltpu.SemaphoreType.DMA((2, length - 1, count + 2)),
            pltpu.SemaphoreType.DMA((2, length - 1, count + 2)),
            pltpu.SemaphoreType.DMA((keys,)),
            pltpu.SemaphoreType.DMA((keys,)),
        ]
        + swap_scratch(n, swaps),
        compiler_params=pltpu.CompilerParams(collective_id=10 + ident, has_side_effects=True),
        cost_estimate=wire_cost(n * rows * columns * 2),
        name="scatter_rows",
    )(partial, *swaps)


def small_gather_kernel(n, a_ref, b_ref, a_out, b_out, send, recv):
    me = lax.axis_index("shard")
    barrier = pltpu.get_barrier_semaphore()
    peers = [lax.rem(me + d, n) for d in range(1, n)]
    for peer in peers:
        pl.semaphore_signal(barrier, inc=1, device_id={"shard": peer}, device_id_type=MESH)
    pl.semaphore_wait(barrier, n - 1)
    copies = Copies()
    for d, peer in enumerate(peers):
        for k, (src, dst) in enumerate(((a_ref, a_out), (b_ref, b_out))):
            copies.start(None, src, dst.at[me], send.at[k, d], recv.at[k, d], peer)
    a_out[me] = a_ref[...]
    b_out[me] = b_ref[...]
    for d in range(1, n):
        source = lax.rem(me + n - d, n)
        for k, dst in enumerate((a_out, b_out)):
            wait_arrival(dst.at[source], send.at[k, d - 1], recv.at[k, d - 1], source)
    copies.finish()


def gather_small(gains, segment_ids):
    n = lax.axis_size("shard")
    width, length = gains.shape[1], segment_ids.shape[1]
    if not use_kernels(n, 256) or width % 128 or length % 128:
        gains = lax.all_gather(gains, "shard", axis=1, tiled=True)
        return gains, lax.all_gather(segment_ids, "shard", axis=0, tiled=True)
    gains = jnp.pad(gains.astype(jnp.float32), ((0, 6), (0, 0)))
    ids = jnp.broadcast_to(segment_ids, (8, length))
    all_gains, all_ids = pl.pallas_call(
        functools.partial(small_gather_kernel, n),
        out_shape=(
            jax.ShapeDtypeStruct((n, 8, width), jnp.float32),
            jax.ShapeDtypeStruct((n, 8, length), jnp.int32),
        ),
        in_specs=[pl.BlockSpec(memory_space=pltpu.VMEM)] * 2,
        out_specs=[pl.BlockSpec(memory_space=pltpu.VMEM)] * 2,
        scratch_shapes=[pltpu.SemaphoreType.DMA((2, n - 1)), pltpu.SemaphoreType.DMA((2, n - 1))],
        compiler_params=pltpu.CompilerParams(collective_id=1, has_side_effects=True),
        name="gather_small",
    )(gains, ids)
    return all_gains[:, :2].transpose(1, 0, 2).reshape(2, n * width), all_ids[:, 0]


def small_sum_kernel(n, m, t_ref, o_ref, got, mine, shared, send, recv, send_two, recv_two):
    me, copy = lax.axis_index("shard"), lax.axis_index("replica")
    barrier = pltpu.get_barrier_semaphore()
    peers = [lax.rem(me + d, n) for d in range(1, n)]
    twins = [lax.rem(copy + d, m) for d in range(1, m)]
    for peer in peers:
        pl.semaphore_signal(barrier, inc=1, device_id={"shard": peer}, device_id_type=MESH)
    for twin in twins:
        pl.semaphore_signal(barrier, inc=1, device_id={"replica": twin}, device_id_type=MESH)
    pl.semaphore_wait(barrier, n + m - 2)
    copies = Copies()
    for d, peer in enumerate(peers):
        copies.start(None, t_ref.at[peer], got.at[me], send.at[d], recv.at[d], peer)
    got[me] = t_ref[me]
    for d in range(1, n):
        source = lax.rem(me + n - d, n)
        wait_arrival(got.at[source], send.at[d - 1], recv.at[d - 1], source)
    total = got[0]
    for i in range(1, n):
        total = total + got[i]
    mine[...] = total
    shared[copy] = total
    for d, twin in enumerate(twins):
        copies.start(
            None, mine, shared.at[copy], send_two.at[d], recv_two.at[d], twin, axis="replica"
        )
    for d in range(1, m):
        source = lax.rem(copy + m - d, m)
        wait_arrival(
            shared.at[source], send_two.at[d - 1], recv_two.at[d - 1], source, axis="replica"
        )
    total = shared[0]
    for i in range(1, m):
        total = total + shared[i]
    o_ref[...] = total
    copies.finish()


def sum_small(terms):
    n, m = lax.axis_size("shard"), lax.axis_size("replica")
    width = terms.shape[1] // n
    if not use_kernels(n, 256) or width % 128:
        total = lax.psum(terms, ("replica", "shard"))
        return lax.dynamic_slice_in_dim(total, lax.axis_index("shard") * width, width, axis=1)
    pieces = jnp.pad(terms, ((0, 6), (0, 0))).reshape(8, n, width).transpose(1, 0, 2)
    return pl.pallas_call(
        functools.partial(small_sum_kernel, n, m),
        out_shape=jax.ShapeDtypeStruct((8, width), jnp.float32),
        in_specs=[pl.BlockSpec(memory_space=pltpu.VMEM)],
        out_specs=pl.BlockSpec(memory_space=pltpu.VMEM),
        scratch_shapes=[
            pltpu.VMEM((n, 8, width), jnp.float32),
            pltpu.VMEM((8, width), jnp.float32),
            pltpu.VMEM((m, 8, width), jnp.float32),
            pltpu.SemaphoreType.DMA((n - 1,)),
            pltpu.SemaphoreType.DMA((n - 1,)),
            pltpu.SemaphoreType.DMA((m - 1,)),
            pltpu.SemaphoreType.DMA((m - 1,)),
        ],
        compiler_params=pltpu.CompilerParams(collective_id=2, has_side_effects=True),
        name="sum_small",
    )(pieces)[:2]


def after(x, *others):
    return lax.optimization_barrier((x,) + others)[0]


def quarters(weights):
    n, copies = lax.axis_size("shard"), lax.axis_size("replica")
    part = weights[0].shape[0] // copies
    me = lax.axis_index("replica")
    pieces = [
        lax.dynamic_slice_in_dim(w, me * part, part).reshape(part, n, -1).transpose(1, 0, 2)
        for w in weights
    ]
    return jnp.concatenate(pieces, axis=2)


def stack_kernel(x_ref, o_ref):
    copies, _, part, _ = x_ref.shape
    for r in range(copies):
        o_ref[pl.ds(r * part, part)] = x_ref[r, 0]


def as_columns(shared):
    copies, n, part, width = shared.shape
    rows = copies * part
    if part % 16 or width % 128:
        return shared.transpose(1, 0, 2, 3).reshape(n * rows, width)
    return pl.pallas_call(
        stack_kernel,
        grid=(n,),
        out_shape=jax.ShapeDtypeStruct((n * rows, width), shared.dtype),
        in_specs=[pl.BlockSpec((copies, 1, part, width), lambda i: (0, i, 0, 0))],
        out_specs=pl.BlockSpec((rows, width), lambda i: (i, 0)),
        name="stack",
    )(shared)


def share(swapped):
    return lax.all_gather(swapped, "replica", axis=0, tiled=False)


def sum_copies(grads):
    n, copies = lax.axis_size("shard"), lax.axis_size("replica")
    rows, width = grads.shape[0] // n, grads.shape[1]
    split = grads.reshape(n, copies, rows // copies, width).transpose(1, 0, 2, 3)
    return lax.psum_scatter(split, "replica", scatter_dimension=0, tiled=False)


def unpack_kernel(widths, x_ref, *o_refs):
    copies, _, part, _ = x_ref.shape
    at = 0
    for width, o_ref in zip(widths, o_refs):
        for r in range(copies):
            o_ref[pl.ds(r * part, part)] = x_ref[r, 0, :, pl.ds(at, width)].astype(o_ref.dtype)
        at += width


def unpack(shared, widths):
    copies, n, part, total = shared.shape
    rows = copies * part
    if part % 16 == 0 and all(width % 128 == 0 for width in widths):
        return pl.pallas_call(
            functools.partial(unpack_kernel, widths),
            grid=(n,),
            out_shape=[jax.ShapeDtypeStruct((rows, n * width), jnp.float32) for width in widths],
            in_specs=[pl.BlockSpec((copies, 1, part, total), lambda i: (0, i, 0, 0))],
            out_specs=[pl.BlockSpec((rows, width), lambda i: (0, i)) for width in widths],
            name="unpack",
        )(shared)
    out, at = [], 0
    for width in widths:
        piece = shared[..., at : at + width].transpose(0, 2, 1, 3).reshape(rows, n * width)
        out.append(piece.astype(jnp.float32))
        at += width
    return out


def positions_tables(segment_rows, head_dim):
    length_all = segment_rows.shape[1]
    counter = lax.broadcasted_iota(jnp.int32, segment_rows.shape, 1)
    is_first = jnp.concatenate(
        [
            jnp.ones((segment_rows.shape[0], 1), jnp.bool_),
            segment_rows[:, 1:] != segment_rows[:, :-1],
        ],
        axis=1,
    )
    first_at = lax.cummax(jnp.where(is_first, counter, jnp.zeros_like(counter)), axis=1)
    position = (counter - first_at).astype(jnp.float32).reshape(-1)
    half_dim = head_dim // 2
    inverse = jnp.exp(
        -(jnp.arange(half_dim, dtype=jnp.float32) * (2.0 / head_dim)) * math.log(THETA)
    )
    angles = position[:, None] * inverse[None, :]
    return (jnp.cos(angles), jnp.sin(angles))


def rotate(values, cosine, sine_tab, direction, head_dim):
    row_count, total_width = values.shape
    half_dim = head_dim // 2
    halves = values.reshape(row_count, total_width // head_dim, 2, half_dim)
    first_half = halves[:, :, 0]
    second_half = halves[:, :, 1]
    cos_wide = cosine[:, None, :]
    sin_wide = direction * sine_tab[:, None, :]
    turned = jnp.stack(
        [
            first_half * cos_wide - second_half * sin_wide,
            second_half * cos_wide + first_half * sin_wide,
        ],
        axis=2,
    )
    return turned.reshape(row_count, total_width)


def allowed(segment_rows):
    ids = jnp.arange(segment_rows.shape[1], dtype=jnp.int32)
    return (segment_rows[:, :, None] == segment_rows[:, None, :]) & (
        ids[None, None, :] <= ids[None, :, None]
    )


def heads_of(values, packs, head_dim):
    return values.reshape(packs, values.shape[0] // packs, -1, head_dim)


def pair_scores(q_heads, k_heads, mask):
    scores = (
        jnp.einsum("pqhd,pkhd->phqk", q_heads, k_heads, preferred_element_type=jnp.float32) * SCALE
    )
    return jnp.where(mask[:, None], scores, -1e30)


def attention_forward(q_rot, k_rot, v_vals, segment_rows, head_dim):
    packs = segment_rows.shape[0]
    q_heads, k_heads, v_heads = (heads_of(v, packs, head_dim) for v in (q_rot, k_rot, v_vals))
    scores = pair_scores(q_heads, k_heads, allowed(segment_rows))
    log_total = jnp.log(jnp.sum(jnp.exp(scores), axis=-1))
    rounded_probs = jnp.exp(scores - log_total[..., None]).astype(jnp.bfloat16)
    mixed_out = jnp.einsum(
        "phqk,pkhd->pqhd", rounded_probs, v_heads, preferred_element_type=jnp.float32
    )
    return mixed_out.astype(jnp.bfloat16).reshape(q_rot.shape), log_total


def attention_backward(q_rot, k_rot, v_vals, log_total, grad_att, segment_rows, head_dim):
    packs = segment_rows.shape[0]
    q_heads, k_heads, v_heads, g_heads = (
        heads_of(v, packs, head_dim) for v in (q_rot, k_rot, v_vals, grad_att)
    )
    scores = pair_scores(q_heads, k_heads, allowed(segment_rows))
    attn_probs = jnp.exp(scores - log_total[..., None])
    grad_probs = jnp.einsum("pqhd,pkhd->phqk", g_heads, v_heads, preferred_element_type=jnp.float32)
    inner_sum = jnp.sum(attn_probs * grad_probs, axis=-1, keepdims=True)
    grad_scores = (attn_probs * (grad_probs - inner_sum) * SCALE).astype(jnp.bfloat16)
    rounded_probs = attn_probs.astype(jnp.bfloat16)
    grad_q = jnp.einsum("phqk,pkhd->pqhd", grad_scores, k_heads, preferred_element_type=jnp.float32)
    grad_k = jnp.einsum("phqk,pqhd->pkhd", grad_scores, q_heads, preferred_element_type=jnp.float32)
    grad_v = jnp.einsum(
        "phqk,pqhd->pkhd", rounded_probs, g_heads, preferred_element_type=jnp.float32
    )
    return tuple(g.reshape(q_rot.shape) for g in (grad_q, grad_k, grad_v))


def turn(values, cosine, sine_tab, direction):
    lane = lax.broadcasted_iota(jnp.int32, values.shape, 1)
    is_first = lane % HEAD_DIM < HEAD_DIM // 2
    width = values.shape[1]
    swapped = jnp.where(
        is_first,
        pltpu.roll(values, width - HEAD_DIM // 2, 1),
        pltpu.roll(values, HEAD_DIM // 2, 1),
    )
    return values * cosine + swapped * jnp.where(is_first, -direction, direction) * sine_tab


def head_probs(q_head, k_head, mask):
    scores = jnp.where(mask, times_transposed(q_head, k_head) * SCALE, -1e30)
    log_total = jnp.log(jnp.sum(jnp.exp(scores), axis=-1, keepdims=True))
    return jnp.exp(scores - log_total)


def attend_kernel(width, qkv_ref, cos_ref, sin_ref, mask_ref, rot_ref, att_ref):
    cosine, sine_tab = cos_ref[...], sin_ref[...]
    mask = mask_ref[0] > 0.5
    lanes = 2 * HEAD_DIM
    for at in range(0, width, lanes):
        q_two = turn(qkv_ref[:, at : at + lanes], cosine, sine_tab, 1.0).astype(jnp.bfloat16)
        k_at, v_at = width + at, 2 * width + at
        k_two = turn(qkv_ref[:, k_at : k_at + lanes], cosine, sine_tab, 1.0).astype(jnp.bfloat16)
        v_two = qkv_ref[:, v_at : v_at + lanes].astype(jnp.bfloat16)
        rot_ref[:, at : at + lanes] = q_two
        rot_ref[:, k_at : k_at + lanes] = k_two
        rot_ref[:, v_at : v_at + lanes] = v_two
        mixed = []
        for h in range(0, lanes, HEAD_DIM):
            one = slice(h, h + HEAD_DIM)
            probs = head_probs(q_two[:, one], k_two[:, one], mask).astype(jnp.bfloat16)
            mixed.append(times_plain(probs, v_two[:, one]))
        att_ref[:, at : at + lanes] = jnp.concatenate(mixed, axis=1).astype(att_ref.dtype)


def attend_back_kernel(width, rot_ref, g_ref, cos_ref, sin_ref, mask_ref, back_ref):
    cosine, sine_tab = cos_ref[...], sin_ref[...]
    mask = mask_ref[0] > 0.5
    lanes = 2 * HEAD_DIM
    for at in range(0, width, lanes):
        k_at, v_at = width + at, 2 * width + at
        q_two = rot_ref[:, at : at + lanes]
        k_two = rot_ref[:, k_at : k_at + lanes]
        v_two = rot_ref[:, v_at : v_at + lanes]
        g_two = g_ref[:, at : at + lanes]
        grads = ([], [], [])
        for h in range(0, lanes, HEAD_DIM):
            one = slice(h, h + HEAD_DIM)
            q, k, v, g = q_two[:, one], k_two[:, one], v_two[:, one], g_two[:, one]
            probs = head_probs(q, k, mask)
            grad_probs = times_transposed(g, v)
            inner = jnp.sum(probs * grad_probs, axis=-1, keepdims=True)
            grad_scores = (probs * (grad_probs - inner) * SCALE).astype(jnp.bfloat16)
            grads[0].append(times_plain(grad_scores, k))
            grads[1].append(token_contract(grad_scores, q))
            grads[2].append(token_contract(probs.astype(jnp.bfloat16), g))
        grad_q, grad_k, grad_v = (jnp.concatenate(g, axis=1) for g in grads)
        dtype = back_ref.dtype
        back_ref[:, at : at + lanes] = turn(grad_q, cosine, sine_tab, -1.0).astype(dtype)
        back_ref[:, k_at : k_at + lanes] = turn(grad_k, cosine, sine_tab, -1.0).astype(dtype)
        back_ref[:, v_at : v_at + lanes] = grad_v.astype(dtype)


def pack_specs(length, *widths):
    return [pl.BlockSpec((length, width), lambda i: (i, 0)) for width in widths]


def wide_tables(segment_rows):
    cosine, sine_tab = positions_tables(segment_rows, HEAD_DIM)
    mask = allowed(segment_rows).astype(jnp.float32)
    return jnp.tile(cosine, (1, 4)), jnp.tile(sine_tab, (1, 4)), mask


def attend(qkv, tables):
    cosine, sine_tab, mask = tables
    packs, length, _ = mask.shape
    tokens, width = qkv.shape[0], qkv.shape[1] // 3
    return pl.pallas_call(
        functools.partial(attend_kernel, width),
        grid=(packs,),
        out_shape=[
            jax.ShapeDtypeStruct((tokens, 3 * width), jnp.bfloat16),
            jax.ShapeDtypeStruct((tokens, width), jnp.bfloat16),
        ],
        in_specs=pack_specs(length, 3 * width, 2 * HEAD_DIM, 2 * HEAD_DIM)
        + [pl.BlockSpec((1, length, length), lambda i: (i, 0, 0))],
        out_specs=pack_specs(length, 3 * width, width),
        name="attend",
    )(qkv, cosine, sine_tab, mask)


def attend_back(rotated, grad_att, tables):
    cosine, sine_tab, mask = tables
    packs, length, _ = mask.shape
    tokens, width = grad_att.shape
    return pl.pallas_call(
        functools.partial(attend_back_kernel, width),
        grid=(packs,),
        out_shape=jax.ShapeDtypeStruct((tokens, 3 * width), jnp.bfloat16),
        in_specs=pack_specs(length, 3 * width, width, 2 * HEAD_DIM, 2 * HEAD_DIM)
        + [pl.BlockSpec((1, length, length), lambda i: (i, 0, 0))],
        out_specs=pack_specs(length, 3 * width)[0],
        name="attend_back",
    )(rotated, grad_att, cosine, sine_tab, mask)


def attend_plain(qkv, segment_rows):
    width = qkv.shape[1] // 3
    cosine, sine_tab = positions_tables(segment_rows, HEAD_DIM)
    q_rot = rotate(qkv[:, :width], cosine, sine_tab, 1.0, HEAD_DIM).astype(jnp.bfloat16)
    k_rot = rotate(qkv[:, width : 2 * width], cosine, sine_tab, 1.0, HEAD_DIM).astype(jnp.bfloat16)
    v_vals = qkv[:, 2 * width :].astype(jnp.bfloat16)
    attended, log_total = attention_forward(q_rot, k_rot, v_vals, segment_rows, HEAD_DIM)
    return (q_rot, k_rot, v_vals, log_total), attended


def attend_back_plain(rotated, grad_att, segment_rows):
    cosine, sine_tab = positions_tables(segment_rows, HEAD_DIM)
    q_rot, k_rot, v_vals, log_total = rotated
    grad_q, grad_k, grad_v = attention_backward(
        q_rot, k_rot, v_vals, log_total, grad_att, segment_rows, HEAD_DIM
    )
    q_back = rotate(grad_q, cosine, sine_tab, -1.0, HEAD_DIM)
    k_back = rotate(grad_k, cosine, sine_tab, -1.0, HEAD_DIM)
    return jnp.concatenate([q_back, k_back, grad_v], axis=1).astype(jnp.bfloat16)


def norm_scale(values):
    return lax.rsqrt(jnp.mean(values * values, axis=-1, keepdims=True) + EPS)


def norm_back(upstream, source, scale, gain, grad_normed):
    gain_term = jnp.sum(grad_normed * source * scale, axis=0)
    weighted = gain * grad_normed
    grad = (
        upstream
        + scale * weighted
        - source * (scale * scale * scale) * jnp.mean(weighted * source, axis=-1, keepdims=True)
    )
    return grad, gain_term


def per_device(
    block_input,
    segment_ids,
    attn_gain,
    mlp_gain,
    w_query,
    w_key,
    w_value,
    w_out,
    w_gate,
    w_up,
    w_down,
    out_grad,
):
    n = lax.axis_size("shard")
    row_count, model_width = block_input.shape

    def spread(x, ident=1, swaps=()):
        gathered, *swapped = gather_rows(x, ident, swaps)
        gathered = gathered.reshape(n * row_count, -1)
        return (gathered, *swapped) if swaps else gathered

    def collect(partial):
        partial = partial.astype(jnp.bfloat16).reshape(n, row_count, model_width)
        return scatter_rows(partial, 1)[0]

    half = model_width // 2
    qkv_quarter = quarters((w_query, w_key, w_value))
    pair_quarter = quarters((w_gate, w_up))
    head_width, ff_width = qkv_quarter.shape[2] // 3, pair_quarter.shape[2] // 2
    by_kernel = head_width % (2 * HEAD_DIM) == 0
    gains, segment_rows = gather_small(jnp.stack([attn_gain, mlp_gain]), segment_ids)
    gain_one, gain_two = gains[0].astype(jnp.float32), gains[1].astype(jnp.float32)

    input_f = block_input.astype(jnp.float32)
    scale_one = norm_scale(input_f)
    normed_own = (input_f * scale_one * gain_one).astype(jnp.bfloat16)
    first_one, qkv_came, pair_came = spread(normed_own[:, :half], 2, (qkv_quarter, pair_quarter))
    qkv_shared = share(qkv_came)
    second_one = spread(after(normed_own[:, half:], first_one), 3)
    pair_shared = share(pair_came)
    cotangent = lax.all_gather(after(out_grad, second_one), "shard", axis=0, tiled=True)
    qkv_cols = as_columns(qkv_shared)
    qkv = times_plain(first_one, qkv_cols[:half]) + times_plain(second_one, qkv_cols[half:])
    if by_kernel:
        tables = wide_tables(segment_rows)
        rotated, attended = attend(qkv, tables)
    else:
        rotated, attended = attend_plain(qkv, segment_rows)
    residual = input_f + collect(times_plain(attended, w_out))
    pair_cols = as_columns(pair_shared)
    scale_two = norm_scale(residual)
    normed_two = spread((residual * scale_two * gain_two).astype(jnp.bfloat16))
    pair_pre = times_plain(normed_two, pair_cols)
    gate_pre, up_pre = pair_pre[:, :ff_width], pair_pre[:, ff_width:]
    gate_sig = jax.nn.sigmoid(gate_pre)
    silu_val = gate_pre * gate_sig
    hidden_b = (silu_val * up_pre).astype(jnp.bfloat16)

    grad_hidden = times_transposed(cotangent, w_down)
    gate_b = (grad_hidden * up_pre * gate_sig * (1.0 + gate_pre * (1.0 - gate_sig))).astype(
        jnp.bfloat16
    )
    up_b = (grad_hidden * silu_val).astype(jnp.bfloat16)
    pair_b = jnp.concatenate([gate_b, up_b], axis=1)
    pair_sum = sum_copies(token_contract(normed_two, pair_b).astype(jnp.bfloat16))
    block_output = (residual + collect(times_plain(hidden_b, w_down))).astype(jnp.bfloat16)
    grad_down = token_contract(hidden_b, cotangent).astype(jnp.bfloat16)
    grad_down = lax.psum(grad_down, "replica")
    grad_normed_two = collect(times_transposed(after(pair_b, block_output), pair_cols))
    grad_residual, gain_two_term = norm_back(
        out_grad.astype(jnp.float32), residual, scale_two, gain_two, grad_normed_two
    )
    residual_own = after(grad_residual.astype(jnp.bfloat16), grad_down)
    residual_b, pair_came = spread(residual_own, 4, (pair_sum,))
    pair_shared = share(pair_came)
    grad_att = times_transposed(residual_b, w_out).astype(jnp.bfloat16)
    if by_kernel:
        back = attend_back(rotated, grad_att, tables)
    else:
        back = attend_back_plain(rotated, grad_att, segment_rows)
    qkv_sum = sum_copies(
        jnp.concatenate([token_contract(first_one, back), token_contract(second_one, back)]).astype(
            jnp.bfloat16
        )
    )
    grad_out = token_contract(attended, residual_b).astype(jnp.bfloat16)
    partial_one = times_transposed(back, qkv_cols).astype(jnp.bfloat16)
    partial_one = partial_one.reshape(n, row_count, model_width)
    (piece_a,) = scatter_rows(after(partial_one[:, :, :half], pair_shared), 2)
    piece_b, qkv_came = scatter_rows(after(partial_one[:, :, half:], piece_a), 3, (qkv_sum,))
    grad_out = lax.psum(after(grad_out, qkv_sum, piece_a, grad_down), "replica")
    qkv_shared = share(qkv_came)
    grad_normed_one = jnp.concatenate([piece_a, piece_b], axis=1)
    input_grad, gain_one_term = norm_back(
        grad_residual, input_f, scale_one, gain_one, grad_normed_one
    )
    gain_rows = sum_small(jnp.stack([gain_one_term, gain_two_term]))
    grad_gate, grad_up = unpack(pair_shared, (ff_width, ff_width))
    grad_query, grad_key, grad_value = unpack(qkv_shared, (head_width,) * 3)
    return (
        block_output,
        input_grad,
        grad_query,
        grad_key,
        grad_value,
        grad_out.astype(jnp.float32),
        grad_gate,
        grad_up,
        grad_down.astype(jnp.float32),
        gain_rows[0],
        gain_rows[1],
    )


def solution(mesh):
    placed = (
        P(("replica", "shard"), None),
        P(("replica", "shard"), None),
        P("shard"),
        P("shard"),
        P("shard", None),
        P("shard", None),
        P("shard", None),
        P("shard", None),
        P("shard", None),
        P("shard", None),
        P("shard", None),
        P(("replica", "shard"), None),
    )
    return jax.shard_map(
        per_device,
        mesh=mesh,
        in_specs=placed,
        out_specs=(
            P(("replica", "shard"), None),
            P(("replica", "shard"), None),
            P("shard", None),
            P("shard", None),
            P("shard", None),
            P("shard", None),
            P("shard", None),
            P("shard", None),
            P("shard", None),
            P("shard"),
            P("shard"),
        ),
        check_vma=False,
    )
```

```python
import functools
import math

import jax
import jax.numpy as jnp
from jax import lax
from jax.experimental import pallas as pl
from jax.experimental.pallas import tpu as pltpu
from jax.sharding import PartitionSpec as P

MESH = pl.DeviceIdType.MESH

HEAD_DIM = 64


EPS = 1e-05
THETA = 130000.0
SCALE = 0.125


def times_plain(left_op, right_op):
    return jnp.dot(left_op, right_op, preferred_element_type=jnp.float32)


def times_transposed(left_op, right_op):
    return lax.dot_general(
        left_op, right_op, (((1,), (1,)), ((), ())), preferred_element_type=jnp.float32
    )


def token_contract(left_op, right_op):
    return lax.dot_general(
        left_op, right_op, (((0,), (0,)), ((), ())), preferred_element_type=jnp.float32
    )


def split_rows(rows, sixteenths=3):
    unit = 16
    across = (rows // unit) * sixteenths // 16 * unit
    rest = (rows - across) // unit
    count = min(4, rest)
    sizes = [(rest // count + (1 if i >= count - rest % count else 0)) * unit for i in range(count)]
    chunks, at = [], across
    for size in sizes:
        chunks.append((at, size))
        at += size
    return across, chunks


def use_kernels(n, rows):
    return n % 2 == 0 and 2 < n <= 8 and rows % 256 == 0


def wire_cost(size):
    return pl.CostEstimate(flops=0, bytes_accessed=30 * size, transcendentals=0)


class Copies:
    def __init__(self):
        self.started = []

    def start(self, cond, src, dst, send_sem, recv_sem, target, axis="shard"):
        copy = pltpu.make_async_remote_copy(
            src_ref=src,
            dst_ref=dst,
            send_sem=send_sem,
            recv_sem=recv_sem,
            device_id={axis: target},
            device_id_type=MESH,
        )
        if cond is None:
            copy.start()
        else:
            pl.when(cond)(copy.start)
        self.started.append((cond, copy))

    def finish(self):
        for cond, copy in self.started:
            if cond is None:
                copy.wait_send()
            else:
                pl.when(cond)(copy.wait_send)


def wait_arrival(dst, send_sem, recv_sem, source, axis="shard"):
    pltpu.make_async_remote_copy(
        src_ref=dst,
        dst_ref=dst,
        send_sem=send_sem,
        recv_sem=recv_sem,
        device_id={axis: source},
        device_id_type=MESH,
    ).wait_recv()


def greet_all(n, me):
    barrier = pltpu.get_barrier_semaphore()
    for d in range(1, n):
        pl.semaphore_signal(
            barrier, inc=1, device_id={"shard": lax.rem(me + d, n)}, device_id_type=MESH
        )
    pl.semaphore_wait(barrier, n - 1)


class Swaps:
    def __init__(self, n, me, sources, targets, send, recv):
        self.n, self.me, self.send, self.recv = n, me, send, recv
        self.pairs = list(zip(sources, targets))

    def start(self, copies):
        for d in range(1, self.n):
            peer = lax.rem(self.me + d, self.n)
            for k, (source, target) in enumerate(self.pairs):
                copies.start(
                    None,
                    source.at[peer],
                    target.at[self.me],
                    self.send.at[k, d - 1],
                    self.recv.at[k, d - 1],
                    peer,
                )
        for source, target in self.pairs:
            target[self.me] = source[self.me]

    def wait(self):
        for d in range(1, self.n):
            sender = lax.rem(self.me + self.n - d, self.n)
            for k, (_, target) in enumerate(self.pairs):
                wait_arrival(
                    target.at[sender], self.send.at[k, d - 1], self.recv.at[k, d - 1], sender
                )


def swap_scratch(n, swaps):
    return [pltpu.SemaphoreType.DMA((max(len(swaps), 1), n - 1))] * 2


def swap_plain(swaps):
    return [lax.all_to_all(s, "shard", split_axis=0, concat_axis=0, tiled=True) for s in swaps]


def greet(has_left, has_right, left, right, other):
    barrier = pltpu.get_barrier_semaphore()
    pl.semaphore_signal(barrier, inc=1, device_id={"shard": other}, device_id_type=MESH)

    @pl.when(has_left)
    def _():
        pl.semaphore_signal(barrier, inc=1, device_id={"shard": left}, device_id_type=MESH)

    @pl.when(has_right)
    def _():
        pl.semaphore_signal(barrier, inc=1, device_id={"shard": right}, device_id_type=MESH)

    pl.semaphore_wait(barrier, 1 + has_left.astype(jnp.int32) + has_right.astype(jnp.int32))


def gather_steps(n, across, chunks, copies, x_ref, o_ref, own_sem, z_send, z_recv, y_send, y_recv):
    length = n // 2
    count = len(chunks)
    me = lax.axis_index("shard")
    place, side = me // 2, me % 2
    other = me + 1 - 2 * side
    has_left, has_right = place > 0, place < length - 1
    nexts = ((has_right, me + 2), (has_left, me - 2))
    own = pltpu.make_async_copy(x_ref, o_ref.at[me], own_sem)
    own.start()
    first = pl.ds(0, across)
    y_first = (2 * length - 1) * count
    copies.start(
        None, x_ref.at[first], o_ref.at[me, first], y_send.at[y_first], y_recv.at[y_first], other
    )

    def z_hop(direction, hop, slot, src, dst):
        cond, target = nexts[direction]
        copies.start(
            cond,
            src,
            dst,
            z_send.at[direction, hop, slot],
            z_recv.at[direction, hop, slot],
            target,
        )

    def y_hop(origin, chunk, src, dst, cond, key):
        copies.start(cond, src, dst, y_send.at[key], y_recv.at[key], other)

    for c, (at, size) in enumerate(chunks):
        span = pl.ds(at, size)
        for direction in range(2):
            z_hop(direction, 0, c, x_ref.at[span], o_ref.at[me, span])
        y_hop(me, c, x_ref.at[span], o_ref.at[me, span], None, c)
    yield
    for hop in range(1, length):
        for c, (at, size) in enumerate(chunks):
            span = pl.ds(at, size)
            for direction in range(2):
                source = me - 2 * hop if direction == 0 else me + 2 * hop
                exists = source >= 0 if direction == 0 else source < n
                sender = me - 2 if direction == 0 else me + 2
                yield

                @pl.when(exists)
                def _():
                    wait_arrival(
                        o_ref.at[source, span],
                        z_send.at[direction, hop - 1, c],
                        z_recv.at[direction, hop - 1, c],
                        sender,
                    )

                here = o_ref.at[source, span]
                if hop < length - 1:
                    cond, target = nexts[direction]
                    copies.start(
                        jnp.logical_and(exists, cond),
                        here,
                        here,
                        z_send.at[direction, hop, c],
                        z_recv.at[direction, hop, c],
                        target,
                    )
                key = (1 + direction * (length - 1) + hop - 1) * count + c
                copies.start(exists, here, here, y_send.at[key], y_recv.at[key], other)
    yield
    wait_arrival(o_ref.at[other, first], y_send.at[y_first], y_recv.at[y_first], other)
    for direction in range(2):
        z_hop(direction, 0, count, x_ref.at[first], o_ref.at[me, first])
        z_hop(direction, 0, count + 1, o_ref.at[other, first], o_ref.at[other, first])
    for hop in range(1, length):
        for line, base in enumerate((me, other)):
            for direction in range(2):
                source = base - 2 * hop if direction == 0 else base + 2 * hop
                exists = source >= 0 if direction == 0 else source < n
                sender = me - 2 if direction == 0 else me + 2
                yield

                @pl.when(exists)
                def _():
                    wait_arrival(
                        o_ref.at[source, first],
                        z_send.at[direction, hop - 1, count + line],
                        z_recv.at[direction, hop - 1, count + line],
                        sender,
                    )

                here = o_ref.at[source, first]
                if hop < length - 1:
                    cond, target = nexts[direction]
                    copies.start(
                        jnp.logical_and(exists, cond),
                        here,
                        here,
                        z_send.at[direction, hop, count + line],
                        z_recv.at[direction, hop, count + line],
                        target,
                    )
    for c, (at, size) in enumerate(chunks):
        span = pl.ds(at, size)
        yield
        wait_arrival(o_ref.at[other, span], y_send.at[c], y_recv.at[c], other)
        for hop in range(1, length):
            for direction in range(2):
                source = other - 2 * hop if direction == 0 else other + 2 * hop
                exists = source >= 0 if direction == 0 else source < n
                key = (1 + direction * (length - 1) + hop - 1) * count + c

                @pl.when(exists)
                def _():
                    wait_arrival(o_ref.at[source, span], y_send.at[key], y_recv.at[key], other)

    own.wait()


def joint_kernel(n, plans, n_swaps, *refs):
    gather_plan, scatter_plan = plans
    refs = list(refs)

    def take(count):
        taken = refs[:count]
        del refs[:count]
        return taken

    x_ref = take(1) if gather_plan else []
    p_ref = take(1) if scatter_plan else []
    swap_in = take(n_swaps)
    x_out = take(1) if gather_plan else []
    p_out = take(1) if scatter_plan else []
    swap_out = take(n_swaps)
    gather_scratch = take(5) if gather_plan else []
    scatter_scratch = take(8) if scatter_plan else []
    me = lax.axis_index("shard")
    place, side = me // 2, me % 2
    if n_swaps:
        greet_all(n, me)
    else:
        greet(place > 0, place < n // 2 - 1, me - 2, me + 2, me + 1 - 2 * side)
    copies = Copies()
    running = []
    if scatter_plan:
        running.append(scatter_steps(n, *scatter_plan, copies, *p_ref, *p_out, *scatter_scratch))
    if gather_plan:
        running.append(gather_steps(n, *gather_plan, copies, *x_ref, *x_out, *gather_scratch))
    for steps in running:
        next(steps)
    swaps = Swaps(n, me, swap_in, swap_out, *(refs or (None, None)))
    if n_swaps:
        swaps.start(copies)
    while running:
        for steps in list(running):
            if next(steps, "end") == "end":
                running.remove(steps)
    if n_swaps:
        swaps.wait()
    copies.finish()


def joint(x, partial, ident, swaps=()):
    n = lax.axis_size("shard")
    rows = (x if partial is None else partial).shape[-2]
    if not use_kernels(n, rows):
        out = []
        if x is not None:
            out.append(lax.all_gather(x, "shard", axis=0, tiled=False))
        if partial is not None:
            flat = partial.reshape(n * rows, partial.shape[2])
            total = lax.psum_scatter(flat, "shard", scatter_dimension=0, tiled=True)
            out.append(total.astype(jnp.float32))
        return *out, *swap_plain(swaps)
    both = x is not None and partial is not None
    across, chunks = split_rows(rows, 6 if both else 3)
    plan = (across, chunks)
    length, count = n // 2, len(chunks)
    keys = (2 * length - 1) * count + 1
    vmem = pl.BlockSpec(memory_space=pltpu.VMEM)
    sems = [
        pltpu.SemaphoreType.DMA((2, length - 1, count + 2)),
        pltpu.SemaphoreType.DMA((2, length - 1, count + 2)),
        pltpu.SemaphoreType.DMA((keys,)),
        pltpu.SemaphoreType.DMA((keys,)),
    ]
    args, out_shape, out_specs, scratch, size = [], [], [], [], 0
    if x is not None:
        args.append(x)
        out_shape.append(jax.ShapeDtypeStruct((n, *x.shape), x.dtype))
        out_specs.append(pl.BlockSpec(memory_space=pl.ANY))
        scratch += [pltpu.SemaphoreType.DMA, *sems]
        size += n * x.size * 2
    if partial is not None:
        columns, dtype = partial.shape[2], partial.dtype
        args.append(partial)
        out_shape.append(jax.ShapeDtypeStruct((rows, columns), jnp.float32))
        out_specs.append(vmem)
        scratch += [
            pltpu.VMEM((2 * length - 1, rows - across, columns), dtype),
            pltpu.VMEM((2, length - 1, across + rows, columns), dtype),
            pltpu.VMEM((across, columns), dtype),
            pltpu.VMEM((across, columns), dtype),
            *sems,
        ]
        size += partial.size * 2
    if swaps:
        scratch += swap_scratch(n, swaps)
    return pl.pallas_call(
        functools.partial(
            joint_kernel,
            n,
            (None if x is None else plan, None if partial is None else plan),
            len(swaps),
        ),
        out_shape=out_shape + [jax.ShapeDtypeStruct(s.shape, s.dtype) for s in swaps],
        in_specs=[vmem] * (len(args) + len(swaps)),
        out_specs=out_specs + [vmem] * len(swaps),
        scratch_shapes=scratch,
        compiler_params=pltpu.CompilerParams(collective_id=2 + ident, has_side_effects=True),
        cost_estimate=wire_cost(size),
        name="joint",
    )(*args, *swaps)


def add_rows(*terms):
    total = terms[0].astype(jnp.float32)
    for term in terms[1:]:
        total = total + term.astype(jnp.float32)
    return total


def scatter_steps(
    n, across, chunks, copies, p_ref, o_ref, y_buf, z_buf, a_buf, a_got, z_send, z_recv, y_send, y_recv
):
    length = n // 2
    count = len(chunks)
    me = lax.axis_index("shard")
    place, side = me // 2, me % 2
    other = me + 1 - 2 * side
    has_left, has_right = place > 0, place < length - 1
    first = pl.ds(0, across)

    def routes():
        for distance in range(length - 1, 0, -1):
            yield 0, distance, place + distance, place + distance < length
            yield 1, distance, place - distance, place - distance >= 0

    behind = (has_left, has_right)
    sender = (me - 2, me + 2)
    target = (me + 2, me - 2)

    for direction, distance, owner, exists in routes():
        for c, (at, size) in enumerate(chunks):
            key = (direction * (length - 1) + distance - 1) * count + c
            copies.start(
                exists,
                p_ref.at[2 * owner + 1 - side, pl.ds(at, size)],
                y_buf.at[direction * (length - 1) + distance - 1, pl.ds(at - across, size)],
                y_send.at[key],
                y_recv.at[key],
                other,
            )
    mid = 2 * (length - 1)
    for c, (at, size) in enumerate(chunks):
        key = mid * count + c
        copies.start(
            None,
            p_ref.at[2 * place + 1 - side, pl.ds(at, size)],
            y_buf.at[mid, pl.ds(at - across, size)],
            y_send.at[key],
            y_recv.at[key],
            other,
        )

    yield

    def z_dst(direction, distance, at, size):
        return z_buf.at[direction, distance, pl.ds(at, size)]

    for direction, distance, owner, exists in routes():
        for line in range(2):
            block = 2 * owner + (side if line == 0 else 1 - side)
            sem_in = (direction, distance, count + line)
            sem_out = (direction, distance - 1, count + line)
            place_rows = line * across
            from_start = jnp.logical_and(exists, jnp.logical_not(behind[direction]))
            passing = jnp.logical_and(exists, behind[direction])
            dst = z_dst(direction, distance - 1, place_rows, across)
            copies.start(
                from_start,
                p_ref.at[block, first],
                dst,
                z_send.at[sem_out],
                z_recv.at[sem_out],
                target[direction],
            )
            if distance < length - 1:
                here = z_dst(direction, distance, place_rows, across)
                yield

                @pl.when(passing)
                def _():
                    wait_arrival(here, z_send.at[sem_in], z_recv.at[sem_in], sender[direction])
                    here[...] = add_rows(here[...], p_ref[block, first]).astype(here.dtype)

                copies.start(
                    passing, here, dst, z_send.at[sem_out], z_recv.at[sem_out], target[direction]
                )

    for line in (1, 0):
        block = 2 * place + (side if line == 0 else 1 - side)
        o_ref[first] = p_ref[block, first].astype(jnp.float32)
        for direction in range(2):
            sem_in = (direction, 0, count + line)
            here = z_dst(direction, 0, line * across, across)
            yield

            @pl.when(behind[direction])
            def _():
                wait_arrival(here, z_send.at[sem_in], z_recv.at[sem_in], sender[direction])
                o_ref[first] = o_ref[first] + here[...].astype(jnp.float32)

        if line == 1:
            a_buf[...] = o_ref[first].astype(a_buf.dtype)
            key = (mid + 1) * count
            copies.start(None, a_buf, a_got, y_send.at[key], y_recv.at[key], other)

    for direction, distance, owner, exists in routes():
        slot = direction * (length - 1) + distance - 1
        for c, (at, size) in enumerate(chunks):
            key = slot * count + c
            held = y_buf.at[slot, pl.ds(at - across, size)]
            block = 2 * owner + side
            sem_in = (direction, distance, c)
            sem_out = (direction, distance - 1, c)
            rows_at = across + at
            span = pl.ds(at, size)
            yield

            @pl.when(exists)
            def _():
                wait_arrival(held, y_send.at[key], y_recv.at[key], other)

            if distance < length - 1:
                here = z_dst(direction, distance, rows_at, size)

                @pl.when(jnp.logical_and(exists, behind[direction]))
                def _():
                    wait_arrival(here, z_send.at[sem_in], z_recv.at[sem_in], sender[direction])
                    held[...] = add_rows(held[...], p_ref[block, span], here[...]).astype(
                        held.dtype
                    )

            @pl.when(jnp.logical_and(exists, jnp.logical_not(behind[direction])))
            def _():
                held[...] = add_rows(held[...], p_ref[block, span]).astype(held.dtype)

            copies.start(
                exists,
                held,
                z_dst(direction, distance - 1, rows_at, size),
                z_send.at[sem_out],
                z_recv.at[sem_out],
                target[direction],
            )
    for c, (at, size) in enumerate(chunks):
        key = mid * count + c
        held = y_buf.at[mid, pl.ds(at - across, size)]
        span = pl.ds(at, size)
        yield
        wait_arrival(held, y_send.at[key], y_recv.at[key], other)
        o_ref[span] = add_rows(held[...], p_ref[me, span])
        for direction in range(2):
            sem_in = (direction, 0, c)
            here = z_dst(direction, 0, across + at, size)

            @pl.when(behind[direction])
            def _():
                wait_arrival(here, z_send.at[sem_in], z_recv.at[sem_in], sender[direction])
                o_ref[span] = o_ref[span] + here[...].astype(jnp.float32)

    key = (mid + 1) * count
    yield
    wait_arrival(a_got, y_send.at[key], y_recv.at[key], other)
    o_ref[first] = o_ref[first] + a_got[...].astype(jnp.float32)


def small_gather_kernel(n, a_ref, b_ref, a_out, b_out, send, recv):
    me = lax.axis_index("shard")
    barrier = pltpu.get_barrier_semaphore()
    peers = [lax.rem(me + d, n) for d in range(1, n)]
    for peer in peers:
        pl.semaphore_signal(barrier, inc=1, device_id={"shard": peer}, device_id_type=MESH)
    pl.semaphore_wait(barrier, n - 1)
    copies = Copies()
    for d, peer in enumerate(peers):
        for k, (src, dst) in enumerate(((a_ref, a_out), (b_ref, b_out))):
            copies.start(None, src, dst.at[me], send.at[k, d], recv.at[k, d], peer)
    a_out[me] = a_ref[...]
    b_out[me] = b_ref[...]
    for d in range(1, n):
        source = lax.rem(me + n - d, n)
        for k, dst in enumerate((a_out, b_out)):
            wait_arrival(dst.at[source], send.at[k, d - 1], recv.at[k, d - 1], source)
    copies.finish()


def gather_small(gains, segment_ids):
    n = lax.axis_size("shard")
    width, length = gains.shape[1], segment_ids.shape[1]
    if not use_kernels(n, 256) or width % 128 or length % 128:
        gains = lax.all_gather(gains, "shard", axis=1, tiled=True)
        return gains, lax.all_gather(segment_ids, "shard", axis=0, tiled=True)
    gains = jnp.pad(gains.astype(jnp.float32), ((0, 6), (0, 0)))
    ids = jnp.broadcast_to(segment_ids, (8, length))
    all_gains, all_ids = pl.pallas_call(
        functools.partial(small_gather_kernel, n),
        out_shape=(
            jax.ShapeDtypeStruct((n, 8, width), jnp.float32),
            jax.ShapeDtypeStruct((n, 8, length), jnp.int32),
        ),
        in_specs=[pl.BlockSpec(memory_space=pltpu.VMEM)] * 2,
        out_specs=[pl.BlockSpec(memory_space=pltpu.VMEM)] * 2,
        scratch_shapes=[pltpu.SemaphoreType.DMA((2, n - 1)), pltpu.SemaphoreType.DMA((2, n - 1))],
        compiler_params=pltpu.CompilerParams(collective_id=0, has_side_effects=True),
        name="gather_small",
    )(gains, ids)
    return all_gains[:, :2].transpose(1, 0, 2).reshape(2, n * width), all_ids[:, 0]


def small_sum_kernel(n, m, t_ref, o_ref, got, mine, shared, send, recv, send_two, recv_two):
    me, copy = lax.axis_index("shard"), lax.axis_index("replica")
    barrier = pltpu.get_barrier_semaphore()
    peers = [lax.rem(me + d, n) for d in range(1, n)]
    twins = [lax.rem(copy + d, m) for d in range(1, m)]
    for peer in peers:
        pl.semaphore_signal(barrier, inc=1, device_id={"shard": peer}, device_id_type=MESH)
    for twin in twins:
        pl.semaphore_signal(barrier, inc=1, device_id={"replica": twin}, device_id_type=MESH)
    pl.semaphore_wait(barrier, n + m - 2)
    copies = Copies()
    for d, peer in enumerate(peers):
        copies.start(None, t_ref.at[peer], got.at[me], send.at[d], recv.at[d], peer)
    got[me] = t_ref[me]
    for d in range(1, n):
        source = lax.rem(me + n - d, n)
        wait_arrival(got.at[source], send.at[d - 1], recv.at[d - 1], source)
    total = got[0]
    for i in range(1, n):
        total = total + got[i]
    mine[...] = total
    shared[copy] = total
    for d, twin in enumerate(twins):
        copies.start(
            None, mine, shared.at[copy], send_two.at[d], recv_two.at[d], twin, axis="replica"
        )
    for d in range(1, m):
        source = lax.rem(copy + m - d, m)
        wait_arrival(
            shared.at[source], send_two.at[d - 1], recv_two.at[d - 1], source, axis="replica"
        )
    total = shared[0]
    for i in range(1, m):
        total = total + shared[i]
    o_ref[...] = total
    copies.finish()


def sum_small(terms):
    n, m = lax.axis_size("shard"), lax.axis_size("replica")
    width = terms.shape[1] // n
    if not use_kernels(n, 256) or width % 128:
        total = lax.psum(terms, ("replica", "shard"))
        return lax.dynamic_slice_in_dim(total, lax.axis_index("shard") * width, width, axis=1)
    pieces = jnp.pad(terms, ((0, 6), (0, 0))).reshape(8, n, width).transpose(1, 0, 2)
    return pl.pallas_call(
        functools.partial(small_sum_kernel, n, m),
        out_shape=jax.ShapeDtypeStruct((8, width), jnp.float32),
        in_specs=[pl.BlockSpec(memory_space=pltpu.VMEM)],
        out_specs=pl.BlockSpec(memory_space=pltpu.VMEM),
        scratch_shapes=[
            pltpu.VMEM((n, 8, width), jnp.float32),
            pltpu.VMEM((8, width), jnp.float32),
            pltpu.VMEM((m, 8, width), jnp.float32),
            pltpu.SemaphoreType.DMA((n - 1,)),
            pltpu.SemaphoreType.DMA((n - 1,)),
            pltpu.SemaphoreType.DMA((m - 1,)),
            pltpu.SemaphoreType.DMA((m - 1,)),
        ],
        compiler_params=pltpu.CompilerParams(collective_id=1, has_side_effects=True),
        name="sum_small",
    )(pieces)[:2]


def after(x, *others):
    return lax.optimization_barrier((x,) + others)[0]


def quarters(weights):
    n, copies = lax.axis_size("shard"), lax.axis_size("replica")
    part = weights[0].shape[0] // copies
    me = lax.axis_index("replica")
    pieces = [
        lax.dynamic_slice_in_dim(w, me * part, part).reshape(part, n, -1).transpose(1, 0, 2)
        for w in weights
    ]
    return jnp.concatenate(pieces, axis=2)


def stack_kernel(x_ref, o_ref):
    copies, _, part, _ = x_ref.shape
    for r in range(copies):
        o_ref[pl.ds(r * part, part)] = x_ref[r, 0]


def as_columns(shared):
    copies, n, part, width = shared.shape
    rows = copies * part
    if part % 16 or width % 128:
        return shared.transpose(1, 0, 2, 3).reshape(n * rows, width)
    return pl.pallas_call(
        stack_kernel,
        grid=(n,),
        out_shape=jax.ShapeDtypeStruct((n * rows, width), shared.dtype),
        in_specs=[pl.BlockSpec((copies, 1, part, width), lambda i: (0, i, 0, 0))],
        out_specs=pl.BlockSpec((rows, width), lambda i: (i, 0)),
        name="stack",
    )(shared)


def share(swapped):
    return lax.all_gather(swapped, "replica", axis=0, tiled=False)


def sum_copies(grads):
    n, copies = lax.axis_size("shard"), lax.axis_size("replica")
    rows, width = grads.shape[0] // n, grads.shape[1]
    split = grads.reshape(n, copies, rows // copies, width).transpose(1, 0, 2, 3)
    return lax.psum_scatter(split, "replica", scatter_dimension=0, tiled=False)


def unpack_kernel(widths, x_ref, *o_refs):
    copies, _, part, _ = x_ref.shape
    at = 0
    for width, o_ref in zip(widths, o_refs):
        for r in range(copies):
            o_ref[pl.ds(r * part, part)] = x_ref[r, 0, :, pl.ds(at, width)].astype(o_ref.dtype)
        at += width


def unpack(shared, widths):
    copies, n, part, total = shared.shape
    rows = copies * part
    if part % 16 == 0 and all(width % 128 == 0 for width in widths):
        return pl.pallas_call(
            functools.partial(unpack_kernel, widths),
            grid=(n,),
            out_shape=[jax.ShapeDtypeStruct((rows, n * width), jnp.float32) for width in widths],
            in_specs=[pl.BlockSpec((copies, 1, part, total), lambda i: (0, i, 0, 0))],
            out_specs=[pl.BlockSpec((rows, width), lambda i: (0, i)) for width in widths],
            name="unpack",
        )(shared)
    out, at = [], 0
    for width in widths:
        piece = shared[..., at : at + width].transpose(0, 2, 1, 3).reshape(rows, n * width)
        out.append(piece.astype(jnp.float32))
        at += width
    return out


def positions_tables(segment_rows, head_dim):
    length_all = segment_rows.shape[1]
    counter = lax.broadcasted_iota(jnp.int32, segment_rows.shape, 1)
    is_first = jnp.concatenate(
        [
            jnp.ones((segment_rows.shape[0], 1), jnp.bool_),
            segment_rows[:, 1:] != segment_rows[:, :-1],
        ],
        axis=1,
    )
    first_at = lax.cummax(jnp.where(is_first, counter, jnp.zeros_like(counter)), axis=1)
    position = (counter - first_at).astype(jnp.float32).reshape(-1)
    half_dim = head_dim // 2
    inverse = jnp.exp(
        -(jnp.arange(half_dim, dtype=jnp.float32) * (2.0 / head_dim)) * math.log(THETA)
    )
    angles = position[:, None] * inverse[None, :]
    return (jnp.cos(angles), jnp.sin(angles))


def rotate(values, cosine, sine_tab, direction, head_dim):
    row_count, total_width = values.shape
    half_dim = head_dim // 2
    halves = values.reshape(row_count, total_width // head_dim, 2, half_dim)
    first_half = halves[:, :, 0]
    second_half = halves[:, :, 1]
    cos_wide = cosine[:, None, :]
    sin_wide = direction * sine_tab[:, None, :]
    turned = jnp.stack(
        [
            first_half * cos_wide - second_half * sin_wide,
            second_half * cos_wide + first_half * sin_wide,
        ],
        axis=2,
    )
    return turned.reshape(row_count, total_width)


def allowed(segment_rows):
    ids = jnp.arange(segment_rows.shape[1], dtype=jnp.int32)
    return (segment_rows[:, :, None] == segment_rows[:, None, :]) & (
        ids[None, None, :] <= ids[None, :, None]
    )


def heads_of(values, packs, head_dim):
    return values.reshape(packs, values.shape[0] // packs, -1, head_dim)


def pair_scores(q_heads, k_heads, mask):
    scores = (
        jnp.einsum("pqhd,pkhd->phqk", q_heads, k_heads, preferred_element_type=jnp.float32) * SCALE
    )
    return jnp.where(mask[:, None], scores, -1e30)


def attention_forward(q_rot, k_rot, v_vals, segment_rows, head_dim):
    packs = segment_rows.shape[0]
    q_heads, k_heads, v_heads = (heads_of(v, packs, head_dim) for v in (q_rot, k_rot, v_vals))
    scores = pair_scores(q_heads, k_heads, allowed(segment_rows))
    log_total = jnp.log(jnp.sum(jnp.exp(scores), axis=-1))
    rounded_probs = jnp.exp(scores - log_total[..., None]).astype(jnp.bfloat16)
    mixed_out = jnp.einsum(
        "phqk,pkhd->pqhd", rounded_probs, v_heads, preferred_element_type=jnp.float32
    )
    return mixed_out.astype(jnp.bfloat16).reshape(q_rot.shape), log_total


def attention_backward(q_rot, k_rot, v_vals, log_total, grad_att, segment_rows, head_dim):
    packs = segment_rows.shape[0]
    q_heads, k_heads, v_heads, g_heads = (
        heads_of(v, packs, head_dim) for v in (q_rot, k_rot, v_vals, grad_att)
    )
    scores = pair_scores(q_heads, k_heads, allowed(segment_rows))
    attn_probs = jnp.exp(scores - log_total[..., None])
    grad_probs = jnp.einsum("pqhd,pkhd->phqk", g_heads, v_heads, preferred_element_type=jnp.float32)
    inner_sum = jnp.sum(attn_probs * grad_probs, axis=-1, keepdims=True)
    grad_scores = (attn_probs * (grad_probs - inner_sum) * SCALE).astype(jnp.bfloat16)
    rounded_probs = attn_probs.astype(jnp.bfloat16)
    grad_q = jnp.einsum("phqk,pkhd->pqhd", grad_scores, k_heads, preferred_element_type=jnp.float32)
    grad_k = jnp.einsum("phqk,pqhd->pkhd", grad_scores, q_heads, preferred_element_type=jnp.float32)
    grad_v = jnp.einsum(
        "phqk,pqhd->pkhd", rounded_probs, g_heads, preferred_element_type=jnp.float32
    )
    return tuple(g.reshape(q_rot.shape) for g in (grad_q, grad_k, grad_v))


def turn(values, cosine, sine_tab, direction):
    lane = lax.broadcasted_iota(jnp.int32, values.shape, 1)
    is_first = lane % HEAD_DIM < HEAD_DIM // 2
    width = values.shape[1]
    swapped = jnp.where(
        is_first,
        pltpu.roll(values, width - HEAD_DIM // 2, 1),
        pltpu.roll(values, HEAD_DIM // 2, 1),
    )
    return values * cosine + swapped * jnp.where(is_first, -direction, direction) * sine_tab


def head_probs(q_head, k_head, mask):
    scores = jnp.where(mask, times_transposed(q_head, k_head) * SCALE, -1e30)
    log_total = jnp.log(jnp.sum(jnp.exp(scores), axis=-1, keepdims=True))
    return jnp.exp(scores - log_total)


def attend_kernel(width, qkv_ref, cos_ref, sin_ref, mask_ref, rot_ref, att_ref):
    cosine, sine_tab = cos_ref[...], sin_ref[...]
    mask = mask_ref[0] > 0.5
    lanes = 2 * HEAD_DIM
    for at in range(0, width, lanes):
        q_two = turn(qkv_ref[:, at : at + lanes], cosine, sine_tab, 1.0).astype(jnp.bfloat16)
        k_at, v_at = width + at, 2 * width + at
        k_two = turn(qkv_ref[:, k_at : k_at + lanes], cosine, sine_tab, 1.0).astype(jnp.bfloat16)
        v_two = qkv_ref[:, v_at : v_at + lanes].astype(jnp.bfloat16)
        rot_ref[:, at : at + lanes] = q_two
        rot_ref[:, k_at : k_at + lanes] = k_two
        rot_ref[:, v_at : v_at + lanes] = v_two
        mixed = []
        for h in range(0, lanes, HEAD_DIM):
            one = slice(h, h + HEAD_DIM)
            probs = head_probs(q_two[:, one], k_two[:, one], mask).astype(jnp.bfloat16)
            mixed.append(times_plain(probs, v_two[:, one]))
        att_ref[:, at : at + lanes] = jnp.concatenate(mixed, axis=1).astype(att_ref.dtype)


def attend_back_kernel(width, rot_ref, g_ref, cos_ref, sin_ref, mask_ref, back_ref):
    cosine, sine_tab = cos_ref[...], sin_ref[...]
    mask = mask_ref[0] > 0.5
    lanes = 2 * HEAD_DIM
    for at in range(0, width, lanes):
        k_at, v_at = width + at, 2 * width + at
        q_two = rot_ref[:, at : at + lanes]
        k_two = rot_ref[:, k_at : k_at + lanes]
        v_two = rot_ref[:, v_at : v_at + lanes]
        g_two = g_ref[:, at : at + lanes]
        grads = ([], [], [])
        for h in range(0, lanes, HEAD_DIM):
            one = slice(h, h + HEAD_DIM)
            q, k, v, g = q_two[:, one], k_two[:, one], v_two[:, one], g_two[:, one]
            probs = head_probs(q, k, mask)
            grad_probs = times_transposed(g, v)
            inner = jnp.sum(probs * grad_probs, axis=-1, keepdims=True)
            grad_scores = (probs * (grad_probs - inner) * SCALE).astype(jnp.bfloat16)
            grads[0].append(times_plain(grad_scores, k))
            grads[1].append(token_contract(grad_scores, q))
            grads[2].append(token_contract(probs.astype(jnp.bfloat16), g))
        grad_q, grad_k, grad_v = (jnp.concatenate(g, axis=1) for g in grads)
        dtype = back_ref.dtype
        back_ref[:, at : at + lanes] = turn(grad_q, cosine, sine_tab, -1.0).astype(dtype)
        back_ref[:, k_at : k_at + lanes] = turn(grad_k, cosine, sine_tab, -1.0).astype(dtype)
        back_ref[:, v_at : v_at + lanes] = grad_v.astype(dtype)


def pack_specs(length, *widths):
    return [pl.BlockSpec((length, width), lambda i: (i, 0)) for width in widths]


def wide_tables(segment_rows):
    cosine, sine_tab = positions_tables(segment_rows, HEAD_DIM)
    mask = allowed(segment_rows).astype(jnp.float32)
    return jnp.tile(cosine, (1, 4)), jnp.tile(sine_tab, (1, 4)), mask


def attend(qkv, tables):
    cosine, sine_tab, mask = tables
    packs, length, _ = mask.shape
    tokens, width = qkv.shape[0], qkv.shape[1] // 3
    return pl.pallas_call(
        functools.partial(attend_kernel, width),
        grid=(packs,),
        out_shape=[
            jax.ShapeDtypeStruct((tokens, 3 * width), jnp.bfloat16),
            jax.ShapeDtypeStruct((tokens, width), jnp.bfloat16),
        ],
        in_specs=pack_specs(length, 3 * width, 2 * HEAD_DIM, 2 * HEAD_DIM)
        + [pl.BlockSpec((1, length, length), lambda i: (i, 0, 0))],
        out_specs=pack_specs(length, 3 * width, width),
        name="attend",
    )(qkv, cosine, sine_tab, mask)


def attend_back(rotated, grad_att, tables):
    cosine, sine_tab, mask = tables
    packs, length, _ = mask.shape
    tokens, width = grad_att.shape
    return pl.pallas_call(
        functools.partial(attend_back_kernel, width),
        grid=(packs,),
        out_shape=jax.ShapeDtypeStruct((tokens, 3 * width), jnp.bfloat16),
        in_specs=pack_specs(length, 3 * width, width, 2 * HEAD_DIM, 2 * HEAD_DIM)
        + [pl.BlockSpec((1, length, length), lambda i: (i, 0, 0))],
        out_specs=pack_specs(length, 3 * width)[0],
        name="attend_back",
    )(rotated, grad_att, cosine, sine_tab, mask)


def attend_plain(qkv, segment_rows):
    width = qkv.shape[1] // 3
    cosine, sine_tab = positions_tables(segment_rows, HEAD_DIM)
    q_rot = rotate(qkv[:, :width], cosine, sine_tab, 1.0, HEAD_DIM).astype(jnp.bfloat16)
    k_rot = rotate(qkv[:, width : 2 * width], cosine, sine_tab, 1.0, HEAD_DIM).astype(jnp.bfloat16)
    v_vals = qkv[:, 2 * width :].astype(jnp.bfloat16)
    attended, log_total = attention_forward(q_rot, k_rot, v_vals, segment_rows, HEAD_DIM)
    return (q_rot, k_rot, v_vals, log_total), attended


def attend_back_plain(rotated, grad_att, segment_rows):
    cosine, sine_tab = positions_tables(segment_rows, HEAD_DIM)
    q_rot, k_rot, v_vals, log_total = rotated
    grad_q, grad_k, grad_v = attention_backward(
        q_rot, k_rot, v_vals, log_total, grad_att, segment_rows, HEAD_DIM
    )
    q_back = rotate(grad_q, cosine, sine_tab, -1.0, HEAD_DIM)
    k_back = rotate(grad_k, cosine, sine_tab, -1.0, HEAD_DIM)
    return jnp.concatenate([q_back, k_back, grad_v], axis=1).astype(jnp.bfloat16)


def norm_scale(values):
    return lax.rsqrt(jnp.mean(values * values, axis=-1, keepdims=True) + EPS)


def norm_back(upstream, source, scale, gain, grad_normed):
    gain_term = jnp.sum(grad_normed * source * scale, axis=0)
    weighted = gain * grad_normed
    grad = (
        upstream
        + scale * weighted
        - source * (scale * scale * scale) * jnp.mean(weighted * source, axis=-1, keepdims=True)
    )
    return grad, gain_term


def per_device(
    block_input,
    segment_ids,
    attn_gain,
    mlp_gain,
    w_query,
    w_key,
    w_value,
    w_out,
    w_gate,
    w_up,
    w_down,
    out_grad,
):
    n = lax.axis_size("shard")
    row_count, model_width = block_input.shape

    def spread(x, ident=1, swaps=()):
        gathered, *swapped = joint(x, None, ident, swaps)
        gathered = gathered.reshape(n * row_count, -1)
        return (gathered, *swapped) if swaps else gathered

    def blocks(partial):
        return partial.astype(jnp.bfloat16).reshape(n, row_count, model_width)

    half = model_width // 2
    qkv_quarter = quarters((w_query, w_key, w_value))
    pair_quarter = quarters((w_gate, w_up))
    head_width, ff_width = qkv_quarter.shape[2] // 3, pair_quarter.shape[2] // 2
    by_kernel = head_width % (2 * HEAD_DIM) == 0
    gains, segment_rows = gather_small(jnp.stack([attn_gain, mlp_gain]), segment_ids)
    gain_one, gain_two = gains[0].astype(jnp.float32), gains[1].astype(jnp.float32)

    input_f = block_input.astype(jnp.float32)
    scale_one = norm_scale(input_f)
    normed_own = (input_f * scale_one * gain_one).astype(jnp.bfloat16)
    first_one, qkv_came, pair_came = spread(normed_own[:, :half], 2, (qkv_quarter, pair_quarter))
    qkv_shared = share(qkv_came)
    second_one = spread(after(normed_own[:, half:], first_one), 3)
    pair_shared = share(pair_came)
    qkv_cols = as_columns(qkv_shared)
    qkv = times_plain(first_one, qkv_cols[:half]) + times_plain(second_one, qkv_cols[half:])
    if by_kernel:
        tables = wide_tables(segment_rows)
        rotated, attended = attend(qkv, tables)
    else:
        rotated, attended = attend_plain(qkv, segment_rows)
    cotangent, attn_rows = joint(out_grad, blocks(times_plain(attended, w_out)), 5)
    cotangent = cotangent.reshape(n * row_count, -1)
    residual = input_f + attn_rows
    pair_cols = as_columns(pair_shared)
    scale_two = norm_scale(residual)
    normed_two = spread((residual * scale_two * gain_two).astype(jnp.bfloat16))
    pair_pre = times_plain(normed_two, pair_cols)
    gate_pre, up_pre = pair_pre[:, :ff_width], pair_pre[:, ff_width:]
    gate_sig = jax.nn.sigmoid(gate_pre)
    silu_val = gate_pre * gate_sig
    hidden_b = (silu_val * up_pre).astype(jnp.bfloat16)

    grad_hidden = times_transposed(cotangent, w_down)
    gate_b = (grad_hidden * up_pre * gate_sig * (1.0 + gate_pre * (1.0 - gate_sig))).astype(
        jnp.bfloat16
    )
    up_b = (grad_hidden * silu_val).astype(jnp.bfloat16)
    pair_b = jnp.concatenate([gate_b, up_b], axis=1)
    pair_sum = sum_copies(token_contract(normed_two, pair_b).astype(jnp.bfloat16))
    mlp_partial = blocks(times_plain(hidden_b, w_down))
    grad_down = token_contract(hidden_b, cotangent).astype(jnp.bfloat16)
    grad_down = lax.psum(grad_down, "replica")
    (grad_normed_two,) = joint(None, blocks(times_transposed(pair_b, pair_cols)), 6)
    grad_residual, gain_two_term = norm_back(
        out_grad.astype(jnp.float32), residual, scale_two, gain_two, grad_normed_two
    )
    residual_b, mlp_rows, pair_came = joint(
        grad_residual.astype(jnp.bfloat16), mlp_partial, 7, (pair_sum,)
    )
    residual_b = residual_b.reshape(n * row_count, -1)
    block_output = (residual + mlp_rows).astype(jnp.bfloat16)
    pair_shared = share(pair_came)
    grad_att = times_transposed(residual_b, w_out).astype(jnp.bfloat16)
    if by_kernel:
        back = attend_back(rotated, grad_att, tables)
    else:
        back = attend_back_plain(rotated, grad_att, segment_rows)
    qkv_sum = sum_copies(
        jnp.concatenate([token_contract(first_one, back), token_contract(second_one, back)]).astype(
            jnp.bfloat16
        )
    )
    grad_out = token_contract(attended, residual_b).astype(jnp.bfloat16)
    partial_one = times_transposed(back, qkv_cols).astype(jnp.bfloat16)
    partial_one = partial_one.reshape(n, row_count, model_width)
    (piece_a,) = joint(None, after(partial_one[:, :, :half], pair_shared, grad_down), 8)
    piece_b, qkv_came = joint(None, after(partial_one[:, :, half:], piece_a), 9, (qkv_sum,))
    grad_out = lax.psum(after(grad_out, qkv_sum, piece_a, grad_down), "replica")
    qkv_shared = share(qkv_came)
    grad_normed_one = jnp.concatenate([piece_a, piece_b], axis=1)
    input_grad, gain_one_term = norm_back(
        grad_residual, input_f, scale_one, gain_one, grad_normed_one
    )
    gain_rows = sum_small(jnp.stack([gain_one_term, gain_two_term]))
    grad_gate, grad_up = unpack(pair_shared, (ff_width, ff_width))
    grad_query, grad_key, grad_value = unpack(qkv_shared, (head_width,) * 3)
    return (
        block_output,
        input_grad,
        grad_query,
        grad_key,
        grad_value,
        grad_out.astype(jnp.float32),
        grad_gate,
        grad_up,
        grad_down.astype(jnp.float32),
        gain_rows[0],
        gain_rows[1],
    )


def solution(mesh):
    placed = (
        P(("replica", "shard"), None),
        P(("replica", "shard"), None),
        P("shard"),
        P("shard"),
        P("shard", None),
        P("shard", None),
        P("shard", None),
        P("shard", None),
        P("shard", None),
        P("shard", None),
        P("shard", None),
        P(("replica", "shard"), None),
    )
    return jax.shard_map(
        per_device,
        mesh=mesh,
        in_specs=placed,
        out_specs=(
            P(("replica", "shard"), None),
            P(("replica", "shard"), None),
            P("shard", None),
            P("shard", None),
            P("shard", None),
            P("shard", None),
            P("shard", None),
            P("shard", None),
            P("shard", None),
            P("shard"),
            P("shard"),
        ),
        check_vma=False,
    )
```
